256 devices in a mesh: grp: 4 (over x), chan: 64 (over y, z, core).
Axes of the slice: x: 4, y: 4, z: 8, core: 2. Of those that a mesh axis runs over, the one named last changes fastest.
Arguments:
- visibility: float32 [1024, 262144], P('chan', 'grp'), may hold values from -6 to 6
- interference_mask: int32 [1024, 131072], P(None, ('grp', 'chan')), may hold values from 0 to 1
- valid_time_count: int32 [4096], P(('grp', 'chan')), may hold values from 8 to 32
- fit_modes: float32 [1024, 32], P('grp'), may hold values from -1 to 1
Outputs:
- residual_vis: float32 [1024, 262144], P('chan', 'grp')
The draws below stay inside these ranges and needn't reach their ends.
All inputs are finite; a program needn't handle non-finite values.
Results may differ from the reference program's by a relative error of at most 0.0003.
Values sent between devices are 32-bit elements; how exact they have to be, the bound alone decides.
A program may use at most 128 MiB of HBM per device.

```python
import jax
import jax.numpy as jnp
from jax import lax

FREQ = 1024
MODES = 32
NT = 32
BASE_DEV = 16
BASE = 4096
N_GRP = 4
N_CHAN = 64


def draw_interference_mask(key, part):
    start_key = jax.random.fold_in(key, 11)
    length_key = jax.random.fold_in(key, 12)
    speck_key = jax.random.fold_in(key, 13)
    columns = BASE * NT
    band_start = jax.random.randint(start_key, (1, columns), 0, FREQ, dtype=jnp.int32)
    band_length = jax.random.randint(length_key, (1, columns), 0, FREQ * 7 // 8 + 1, dtype=jnp.int32)
    freq_index = lax.broadcasted_iota(jnp.int32, (FREQ, columns), 0)
    inside_band = (freq_index >= band_start) & (freq_index < band_start + band_length)
    scattered = jax.random.randint(speck_key, (FREQ, columns), 0, 16, dtype=jnp.int32) == 0
    return (inside_band | scattered).astype(jnp.int32)


def draw_fit_modes(key, part):
    center_key = jax.random.fold_in(key, 21)
    rough_key = jax.random.fold_in(key, 22)
    centers = jax.random.uniform(center_key, (1, MODES), jnp.float32, 0.0, 1.0) * FREQ
    freq_index = lax.broadcasted_iota(jnp.float32, (FREQ, MODES), 0)
    spread = FREQ / 6.0
    offset = (freq_index - centers) / spread
    envelope = 0.25 + 1.75 * jnp.exp(-0.5 * offset * offset)
    rough = jnp.clip(jax.random.normal(rough_key, (FREQ, MODES), jnp.float32), -4.0, 4.0)
    column_scale = jnp.sqrt(jnp.sum(envelope * envelope, axis=0, keepdims=True))
    return jnp.clip(rough * envelope / column_scale, -1.0, 1.0)


def plant(values, own_key, least, top_value):
    extent = values.shape
    index_at = [jax.random.randint(jax.random.fold_in(own_key, axis), (), 0, extent[axis]) for axis in range(len(extent))]
    values = values.at[tuple(index_at)].set(least)
    longest = extent.index(max(extent))
    index_at[longest] = (index_at[longest] + 1) % extent[longest]
    return values.at[tuple(index_at)].set(top_value)


def levels(own_key, shape, pieces, smallest, largest):
    level = 1.0
    for dim, parts in pieces:
        heights = jax.random.uniform(jax.random.fold_in(jax.random.fold_in(own_key, 6), dim), (parts,), jnp.float32, smallest / len(pieces), largest / len(pieces))
        level = level * jnp.repeat(jnp.exp(heights), shape[dim] // parts).reshape((-1,) + (1,) * (len(shape) - 1 - dim))
    return level


def noise(stream_key, dims, width, limit, cuts=(), held_as=jnp.bfloat16):
    values = jax.random.normal(stream_key, dims, jnp.float32) * width
    if len(cuts) > 0:
        values = levels(stream_key, dims, cuts, -0.22, 0.18) * values
    return jnp.clip(values, min=-limit, max=limit).astype(held_as)


def setup_inputs(seed: int = 0) -> dict:
    seeds = jax.random.split(jax.random.key(seed), 5)
    return {
        "visibility": noise(seeds[0], (FREQ, BASE * 2 * NT), 1.0, 6.0, ((0, 64), (1, 4)), jnp.float32),
        "interference_mask": draw_interference_mask(jax.random.fold_in(seeds[4], 71), 0),
        "valid_time_count": plant(jax.random.randint(seeds[2], (BASE,), NT // 4, NT + 1), jax.random.fold_in(seeds[2], 1), NT // 4, NT).astype(jnp.int32),
        "fit_modes": draw_fit_modes(jax.random.fold_in(seeds[4], 71), 0),
    }


damping = 0.1

def fit_weight(interference_mask, valid_time_count):
    antenna_pairs_list = valid_time_count.shape[0]
    sample_values = interference_mask.shape[1] // antenna_pairs_list
    projection_sums = lax.broadcasted_iota(jnp.int32, (antenna_pairs_list, sample_values), 1)
    within_range = (projection_sums < valid_time_count[:, None]).astype(jnp.float32).reshape(1, antenna_pairs_list * sample_values)
    return (1.0 - interference_mask.astype(jnp.float32)) * within_range

def solve_normal(normal_matrix, target_signal):
    span_length = normal_matrix.shape[0]
    trailing = normal_matrix
    columns = []
    for position in range(span_length):
        column = trailing[:, 0] / jnp.sqrt(trailing[0, 0])
        columns.append(column)
        trailing = trailing[1:, 1:] - column[1:, None, :] * column[None, 1:, :]
    remains = target_signal
    forward = []
    for position in range(span_length):
        column = columns[position]
        current = remains[0] / column[0][None, :]
        forward.append(current)
        remains = remains[1:] - column[1:, None, :] * current[None]
    solution_values = [None] * span_length
    for position in reversed(range(span_length)):
        column = columns[position]
        current = forward[position]
        if position + 1 < span_length:
            later_rows = jnp.stack(solution_values[position + 1:], 0)
            current = current - lax.optimization_barrier(jnp.sum(column[1:, None, :] * later_rows, axis=0))
        solution_values[position] = current / column[0][None, :]
    return jnp.stack(solution_values, 0)

def solve_amplitudes(spectral_templates, assigned_rows, sample_weight, antenna_pairs_list):
    channel_count, span_length = spectral_templates.shape
    sample_values = sample_weight.shape[1] // antenna_pairs_list
    pairs = (spectral_templates[:, :, None] * spectral_templates[:, None, :]).reshape(channel_count, span_length * span_length)
    normal_matrix = lax.dot_general(pairs, sample_weight, (((0,), (0,)), ((), ())), precision=lax.Precision.HIGHEST, preferred_element_type=jnp.float32)
    normal_matrix = normal_matrix.reshape(span_length, span_length, antenna_pairs_list * sample_values)
    normal_matrix = normal_matrix + damping * jnp.eye(span_length, dtype=normal_matrix.dtype)[:, :, None]
    weighted_values = assigned_rows.reshape(channel_count, antenna_pairs_list, 2, sample_values) * sample_weight.reshape(channel_count, antenna_pairs_list, 1, sample_values)
    weighted_values = weighted_values.reshape(channel_count, antenna_pairs_list * 2 * sample_values)
    template_projection = lax.dot_general(spectral_templates, weighted_values, (((0,), (0,)), ((), ())), precision=lax.Precision.HIGHEST, preferred_element_type=jnp.float32)
    target_signal = template_projection.reshape(span_length, antenna_pairs_list, 2, sample_values).transpose(0, 2, 1, 3).reshape(span_length, 2, antenna_pairs_list * sample_values)
    solution_values = solve_normal(normal_matrix, target_signal)
    return solution_values.reshape(span_length, 2, antenna_pairs_list, sample_values).transpose(0, 2, 1, 3).reshape(span_length, antenna_pairs_list * 2 * sample_values)

def reference(visibility, interference_mask, valid_time_count, fit_modes):
    blocks = N_GRP * N_CHAN
    stacked = visibility.reshape(FREQ, blocks, BASE_DEV * 2 * NT).transpose(1, 0, 2)
    flagged = interference_mask.reshape(FREQ, blocks, BASE_DEV * NT).transpose(1, 0, 2)
    counted = valid_time_count.reshape(blocks, BASE_DEV)

    def one_block(items):
        assigned_rows, block_flags, block_counts = items
        sample_weight = fit_weight(block_flags, block_counts)
        mode_amplitudes = solve_amplitudes(fit_modes, assigned_rows, sample_weight, BASE_DEV)
        model = jnp.dot(fit_modes, mode_amplitudes, precision=lax.Precision.HIGHEST, preferred_element_type=jnp.float32)
        return assigned_rows - model
    result = lax.map(one_block, (stacked, flagged, counted))
    return result.transpose(1, 0, 2).reshape(FREQ, BASE * 2 * NT)
```

```python
import functools

import jax
import jax.numpy as jnp
from jax import lax
from jax.experimental import pallas as pl
from jax.experimental.pallas import tpu as pltpu
from jax.sharding import PartitionSpec as P

MESH = pl.DeviceIdType.MESH
damping = 0.1

NX = 4
NY = 4
NZ = 8
NC = 2
MODES = 32
LANES = 128
ROWS = 16
SLAB = 256
COLS = 1024
HALF = 512
SEL = NY * NC * ROWS
F32 = jnp.float32
BF16 = jnp.bfloat16


def split(value):
    high = value.astype(BF16)
    low = (value - high.astype(F32)).astype(BF16)
    return high, low


def widen(mask):
    lane = lax.broadcasted_iota(jnp.int32, mask.shape, 1)
    by32 = pltpu.roll(mask, 32, 1)
    by64 = pltpu.roll(mask, 64, 1)
    by96 = pltpu.roll(mask, 96, 1)
    first = jnp.where(lane < 32, mask, jnp.where(lane < 96, by32, by64))
    second = jnp.where(lane < 32, by64, jnp.where(lane < 96, by96, mask))
    return jnp.concatenate([first, second], axis=1)


def dot(a, b):
    return lax.dot_general(a, b, (((1,), (0,)), ((), ())), preferred_element_type=F32)


def fit_kernel(
    vis,
    mask,
    modes,
    valid,
    coef,
    table,
    own_mask,
    got_mask,
    got_vis,
    weight,
    gram,
    flipped,
    chosen,
    partial,
    chain,
    answer,
    own_sem,
    table_sem,
    mask_sem,
    vis_sem,
    chain_sem,
    send_sem,
    chain_send,
):
    x = lax.axis_index("grp")
    chan = lax.axis_index("chan")
    y = chan // (NZ * NC)
    z = (chan // NC) % NZ
    core = chan % NC

    def at(yy, zz, cc):
        return (yy * NZ + zz) * NC + cc

    def ahead(steps):
        return (z + steps + NZ) % NZ

    barrier = pltpu.get_barrier_semaphore()
    for step in range(1, NX):
        pl.semaphore_signal(barrier, 1, device_id={"grp": (x + step) % NX}, device_id_type=MESH)
    for step in range(1, NZ):
        pl.semaphore_signal(barrier, 1, device_id={"chan": at(y, ahead(step), core)}, device_id_type=MESH)
    for step in range(1, NY * NC):
        peer = at((y + step // NC) % NY, z, (core + step) % NC)
        pl.semaphore_signal(barrier, 1, device_id={"chan": peer}, device_id_type=MESH)

    mine = y * NC + core
    local_table = pltpu.make_async_copy(modes, table.at[pl.ds(pl.multiple_of(x * SLAB, SLAB), SLAB)], table_sem.at[0])
    local_table.start()
    local_mask = pltpu.make_async_copy(mask, own_mask, own_sem.at[0])
    local_mask.start()
    pltpu.make_async_copy(mask.at[:, z], got_mask.at[z], mask_sem.at[z]).start()
    for zz in range(NZ):
        source = vis.at[:, pl.ds(pl.multiple_of(at(y, zz, core) * COLS, COLS), COLS)]
        pltpu.make_async_copy(
            source, got_vis.at[zz, pl.ds(pl.multiple_of(mine * ROWS, ROWS), ROWS)], vis_sem.at[zz]
        ).start()

    pl.semaphore_wait(barrier, NX - 1 + NZ - 1 + NY * NC - 1)

    for step in range(1, NX):
        pltpu.make_async_remote_copy(
            src_ref=modes,
            dst_ref=table.at[pl.ds(pl.multiple_of(x * SLAB, SLAB), SLAB)],
            send_sem=send_sem.at[0],
            recv_sem=table_sem.at[1],
            device_id={"grp": (x + step) % NX},
            device_id_type=MESH,
        ).start()

    order = (4, 3, -3, 2, -2, 1, -1)
    for steps in order:
        there = ahead(steps)
        pltpu.make_async_remote_copy(
            src_ref=mask.at[:, there],
            dst_ref=got_mask.at[z],
            send_sem=send_sem.at[1],
            recv_sem=mask_sem.at[z],
            device_id={"chan": at(y, there, core)},
            device_id_type=MESH,
        ).start()
    for steps in order + (0,):
        owner = ahead(steps)
        for step in range(1, NY * NC):
            yy = (y + step // NC) % NY
            cc = (core + step) % NC
            source = vis.at[:, pl.ds(pl.multiple_of(at(yy, owner, cc) * COLS, COLS), COLS)]
            pltpu.make_async_remote_copy(
                src_ref=source,
                dst_ref=got_vis.at[owner, pl.ds(pl.multiple_of(mine * ROWS, ROWS), ROWS)],
                send_sem=send_sem.at[2],
                recv_sem=vis_sem.at[owner],
                device_id={"chan": at(yy, z, cc)},
                device_id_type=MESH,
            ).start()

    local_mask.wait()

    @pl.loop(0, NY * NZ)
    def _(block):
        yy = block // NZ
        zz = block % NZ
        for group in range(HALF // LANES):
            kept = 1 - own_mask[yy, zz, :, group * LANES : (group + 1) * LANES]
            weight[
                pl.ds(pl.multiple_of(block * 32, 32), 32), group * 2 * LANES : (group + 1) * 2 * LANES
            ] = widen(kept.astype(F32)).astype(BF16)

    local_table.wait()
    others = table.at[pl.ds(0, (NX - 1) * SLAB)]
    pltpu.make_async_copy(others, others, table_sem.at[1]).wait()
    flipped[...] = jnp.transpose(table[...])[:MODES]
    rows = [
        table[pl.ds(pl.multiple_of(yy * SLAB + z * NC * ROWS, 32), NC * ROWS), :] for yy in range(NY)
    ]
    high, low = split(jnp.transpose(jnp.concatenate(rows, axis=0))[:MODES])
    chosen[...] = jnp.concatenate([high, high, low], axis=1)

    eye_row = lax.broadcasted_iota(jnp.int32, (MODES, COLS), 0)
    inside = valid[...]

    @pl.loop(0, MODES // 4)
    def _(block):
        pairs = [flipped[...] * flipped[pl.ds(block * 4 + k, 1), :] for k in range(4)]
        high, low = split(jnp.concatenate(pairs, axis=0))
        for part in range(COLS // 256):
            cols = slice(part * 256, (part + 1) * 256)
            held = weight[:, cols]
            sums = (dot(high, held) + dot(low, held)) * inside[:, cols]
            for k in range(4):
                ridge = jnp.where(eye_row[:, cols] == block * 4 + k, damping, 0.0)
                gram[block * 4 + k, :, cols] = sums[k * MODES : (k + 1) * MODES] + ridge

    @pl.loop(0, MODES)
    def _(k):
        scale = lax.rsqrt(gram[k, pl.ds(k, 1), :])
        column = jnp.where(eye_row >= k, gram[k] * scale, 0.0)
        gram[k] = column

        @pl.loop(k + 1, MODES)
        def _(j):
            gram[j] = gram[j] - gram[k] * gram[k, pl.ds(j, 1), :]

    def project(owner, out):
        pltpu.make_async_copy(got_mask.at[owner], got_mask.at[owner], mask_sem.at[owner]).wait()
        pltpu.make_async_copy(got_vis.at[owner], got_vis.at[owner], vis_sem.at[owner]).wait()

        @pl.loop(0, HALF // LANES)
        def _(group):
            narrow = pl.ds(pl.multiple_of(group * LANES, LANES), LANES)
            wide = pl.ds(pl.multiple_of(group * 2 * LANES, 2 * LANES), 2 * LANES)
            flags = jnp.concatenate([got_mask[owner, yy, :, narrow] for yy in range(NY)], axis=0)
            kept = widen((1 - flags).astype(F32))
            high, low = split(kept * got_vis[owner, :, wide])
            out[:, wide] = dot(chosen[...], jnp.concatenate([high, low, high], axis=0))

    def send(way, slot, rows):
        return pltpu.make_async_remote_copy(
            src_ref=partial.at[way, slot, rows],
            dst_ref=chain.at[way, slot, rows],
            send_sem=chain_send.at[way, slot],
            recv_sem=chain_sem.at[way, slot],
            device_id={"chan": at(y, ahead(1 - 2 * way), core)},
            device_id_type=MESH,
        )

    upper = pl.ds(0, MODES // 2)
    lower = pl.ds(MODES // 2, MODES // 2)
    project(ahead(4), partial.at[0, 0])
    partial[1, 0, MODES // 2 :] = partial[0, 0, MODES // 2 :]
    sends = [send(0, 0, upper), send(1, 0, lower)]
    for s in sends:
        s.start()
    everything = pl.ds(0, MODES)
    for slot in range(1, 4):
        for way in range(2):
            project(ahead((4 - slot) * (1 - 2 * way)), partial.at[way, slot])
            if slot == 1:
                piece = (upper, lower)[way]
                sends[way].wait_recv()
                partial[way, slot, piece] = partial[way, slot, piece] + chain[way, 0, piece]
            else:
                sends[(slot - 1) * 2 + way].wait_recv()
                partial[way, slot] = partial[way, slot] + chain[way, slot - 1]
            out = send(way, slot, everything)
            out.start()
            sends.append(out)
    project(z, answer)
    sends[6].wait_recv()
    sends[7].wait_recv()
    answer[...] = (answer[...] + chain[0, 3] + chain[1, 3]) * inside

    @pl.loop(0, MODES)
    def _(k):
        column = gram[k]
        row = answer[pl.ds(k, 1), :] / gram[k, pl.ds(k, 1), :]
        answer[...] = answer[...] - jnp.where(eye_row > k, column * row, 0.0)
        answer[pl.ds(k, 1), :] = row

    coef[...] = jnp.zeros_like(coef)

    @pl.loop(0, MODES)
    def _(step):
        k = MODES - 1 - step
        later = jnp.sum(gram[k] * coef[...], axis=0, keepdims=True)
        coef[pl.ds(k, 1), :] = (answer[pl.ds(k, 1), :] - later) / gram[k, pl.ds(k, 1), :]

    for s in sends:
        s.wait_send()
    sent = table.at[pl.ds(0, (NX - 1) * SLAB)]
    pltpu.make_async_copy(sent, sent, send_sem.at[0]).wait()
    sent = got_mask.at[pl.ds(0, NZ - 1)]
    pltpu.make_async_copy(sent, sent, send_sem.at[1]).wait()
    sent = got_vis.at[pl.ds(0, NY * NC - 1)]
    pltpu.make_async_copy(sent, sent, send_sem.at[2]).wait()


def fit(vis, mask, modes, valid):
    anywhere = pl.BlockSpec(memory_space=pl.ANY)
    held = pl.BlockSpec(memory_space=pltpu.VMEM)
    return pl.pallas_call(
        fit_kernel,
        out_shape=(
            jax.ShapeDtypeStruct((MODES, COLS), F32),
            jax.ShapeDtypeStruct((NX * SLAB, LANES), F32),
        ),
        in_specs=[anywhere, anywhere, anywhere, held],
        out_specs=(held, held),
        scratch_shapes=[
            pltpu.VMEM((NY, NZ, NC * ROWS, HALF), jnp.int32),
            pltpu.VMEM((NZ, NY, NC * ROWS, HALF), jnp.int32),
            pltpu.VMEM((NZ, SEL, COLS), F32),
            pltpu.VMEM((NX * SLAB, COLS), BF16),
            pltpu.VMEM((MODES, MODES, COLS), F32),
            pltpu.VMEM((MODES, NX * SLAB), F32),
            pltpu.VMEM((MODES, 3 * SEL), BF16),
            pltpu.VMEM((2, 4, MODES, COLS), F32),
            pltpu.VMEM((2, 4, MODES, COLS), F32),
            pltpu.VMEM((MODES, COLS), F32),
            pltpu.SemaphoreType.DMA((1,)),
            pltpu.SemaphoreType.DMA((2,)),
            pltpu.SemaphoreType.DMA((NZ,)),
            pltpu.SemaphoreType.DMA((NZ,)),
            pltpu.SemaphoreType.DMA((2, 4)),
            pltpu.SemaphoreType.DMA((3,)),
            pltpu.SemaphoreType.DMA((2, 4)),
        ],
        compiler_params=pltpu.CompilerParams(
            collective_id=0, has_side_effects=True, vmem_limit_bytes=60 * 1024 * 1024
        ),
        name="fit",
    )(vis, mask, modes, valid)


def per_device(visibility, interference_mask, valid_time_count, fit_modes):
    owned = valid_time_count.shape[0]
    times = HALF // owned
    inside = lax.broadcasted_iota(jnp.int32, (owned, 2, times), 2) < valid_time_count[:, None, None]
    valid = inside.astype(F32).reshape(1, COLS)
    modes = jnp.pad(fit_modes, ((0, 0), (0, LANES - MODES)))
    mask = interference_mask.reshape(NY, NZ, NC * ROWS, HALF)
    coef, table = fit(visibility, mask, modes, valid)
    local_rows = visibility.shape[0]
    local_basis = lax.dynamic_slice_in_dim(
        table, lax.axis_index("chan") * local_rows, local_rows, 0
    )[:, :MODES]
    model = jnp.dot(
        local_basis,
        lax.all_gather(coef, "chan", axis=1, tiled=True),
        precision=lax.Precision.HIGHEST,
        preferred_element_type=F32,
    )
    return visibility - model


def solution(mesh):
    placed = (P("chan", "grp"), P(None, ("grp", "chan")), P(("grp", "chan")), P("grp", None))
    return jax.shard_map(
        per_device, mesh=mesh, in_specs=placed, out_specs=P("chan", "grp"), check_vma=False
    )
```

```python
import functools

import jax
import jax.numpy as jnp
from jax import lax
from jax.experimental import pallas as pl
from jax.experimental.pallas import tpu as pltpu
from jax.sharding import PartitionSpec as P

MESH = pl.DeviceIdType.MESH
damping = 0.1

NX = 4
NY = 4
NZ = 8
NC = 2
MODES = 32
LANES = 128
ROWS = 16
SLAB = 256
COLS = 1024
HALF = 512
SEL = NY * NC * ROWS
FIRST, SECOND = slice(0, 512), slice(512, 1024)
FIRST_OF = slice(0, 256), slice(256, 512)
SECOND_OF = slice(512, 768), slice(768, 1024)
F32 = jnp.float32
BF16 = jnp.bfloat16


def split(value):
    high = value.astype(BF16)
    low = (value - high.astype(F32)).astype(BF16)
    return high, low


def widen(mask):
    lane = lax.broadcasted_iota(jnp.int32, mask.shape, 1)
    by32 = pltpu.roll(mask, 32, 1)
    by64 = pltpu.roll(mask, 64, 1)
    by96 = pltpu.roll(mask, 96, 1)
    first = jnp.where(lane < 32, mask, jnp.where(lane < 96, by32, by64))
    second = jnp.where(lane < 32, by64, jnp.where(lane < 96, by96, mask))
    return jnp.concatenate([first, second], axis=1)


def dot(a, b):
    return lax.dot_general(a, b, (((1,), (0,)), ((), ())), preferred_element_type=F32)


def fit_kernel(
    vis,
    mask,
    modes,
    valid,
    out,
    coefs,
    basis,
    kept_vis,
    table,
    own_mask,
    got_mask,
    got_vis,
    weight,
    gram,
    flipped,
    chosen,
    partial,
    chain,
    answer,
    own_sem,
    table_sem,
    mask_sem,
    vis_sem,
    chain_sem,
    send_sem,
    chain_send,
    across_sem,
    along_sem,
    first_sem,
    spread_sem,
    twin_sem,
    load_sem,
    store_sem,
    link_send,
    twin_send,
):
    x = lax.axis_index("grp")
    chan = lax.axis_index("chan")
    y = chan // (NZ * NC)
    z = (chan // NC) % NZ
    core = chan % NC

    def at(yy, zz, cc):
        return (yy * NZ + zz) * NC + cc

    def ahead(steps):
        return (z + steps + NZ) % NZ

    barrier = pltpu.get_barrier_semaphore()
    for step in range(1, NX):
        pl.semaphore_signal(barrier, 1, device_id={"grp": (x + step) % NX}, device_id_type=MESH)
    for step in range(1, NZ):
        pl.semaphore_signal(barrier, 1, device_id={"chan": at(y, ahead(step), core)}, device_id_type=MESH)
    for step in range(1, NY * NC):
        peer = at((y + step // NC) % NY, z, (core + step) % NC)
        pl.semaphore_signal(barrier, 1, device_id={"chan": peer}, device_id_type=MESH)

    mine = y * NC + core
    local_table = pltpu.make_async_copy(modes, table.at[pl.ds(pl.multiple_of(x * SLAB, SLAB), SLAB)], table_sem.at[0])
    local_table.start()
    local_mask = pltpu.make_async_copy(mask, own_mask, own_sem.at[0])
    local_mask.start()
    pltpu.make_async_copy(mask.at[:, z], got_mask.at[z], mask_sem.at[z]).start()
    for zz in range(NZ):
        source = vis.at[:, pl.ds(pl.multiple_of(at(y, zz, core) * COLS, COLS), COLS)]
        pltpu.make_async_copy(
            source, got_vis.at[zz, pl.ds(pl.multiple_of(mine * ROWS, ROWS), ROWS)], vis_sem.at[zz]
        ).start()

    pl.semaphore_wait(barrier, NX - 1 + NZ - 1 + NY * NC - 1)

    for step in range(1, NX):
        pltpu.make_async_remote_copy(
            src_ref=modes,
            dst_ref=table.at[pl.ds(pl.multiple_of(x * SLAB, SLAB), SLAB)],
            send_sem=send_sem.at[0],
            recv_sem=table_sem.at[1],
            device_id={"grp": (x + step) % NX},
            device_id_type=MESH,
        ).start()

    order = (4, 3, -3, 2, -2, 1, -1)
    for steps in order:
        there = ahead(steps)
        pltpu.make_async_remote_copy(
            src_ref=mask.at[:, there],
            dst_ref=got_mask.at[z],
            send_sem=send_sem.at[1],
            recv_sem=mask_sem.at[z],
            device_id={"chan": at(y, there, core)},
            device_id_type=MESH,
        ).start()
    for steps in order + (0,):
        owner = ahead(steps)
        for step in range(1, NY * NC):
            yy = (y + step // NC) % NY
            cc = (core + step) % NC
            source = vis.at[:, pl.ds(pl.multiple_of(at(yy, owner, cc) * COLS, COLS), COLS)]
            pltpu.make_async_remote_copy(
                src_ref=source,
                dst_ref=got_vis.at[owner, pl.ds(pl.multiple_of(mine * ROWS, ROWS), ROWS)],
                send_sem=send_sem.at[2],
                recv_sem=vis_sem.at[owner],
                device_id={"chan": at(yy, z, cc)},
                device_id_type=MESH,
            ).start()

    @pl.loop(0, NY * NZ * NC)
    def _(block):
        source = vis.at[:, pl.ds(pl.multiple_of(block * COLS, COLS), COLS)]
        pltpu.make_async_copy(source, kept_vis.at[block], load_sem.at[0]).start()

    local_mask.wait()

    @pl.loop(0, NY * NZ)
    def _(block):
        yy = block // NZ
        zz = block % NZ
        for group in range(HALF // LANES):
            kept = 1 - own_mask[yy, zz, :, group * LANES : (group + 1) * LANES]
            weight[
                pl.ds(pl.multiple_of(block * 32, 32), 32), group * 2 * LANES : (group + 1) * 2 * LANES
            ] = widen(kept.astype(F32)).astype(BF16)

    local_table.wait()
    others = table.at[pl.ds(0, (NX - 1) * SLAB)]
    pltpu.make_async_copy(others, others, table_sem.at[1]).wait()
    flipped[...] = jnp.transpose(table[...])[:MODES]
    rows = [
        table[pl.ds(pl.multiple_of(yy * SLAB + z * NC * ROWS, 32), NC * ROWS), :] for yy in range(NY)
    ]
    high, low = split(jnp.transpose(jnp.concatenate(rows, axis=0))[:MODES])
    chosen[...] = jnp.concatenate([high, high, low], axis=1)

    high, low = split(table[pl.ds(pl.multiple_of(chan * ROWS, ROWS), ROWS), :][:, :MODES])
    basis[...] = jnp.concatenate([high, high, low], axis=1)

    eye_row = lax.broadcasted_iota(jnp.int32, (MODES, COLS), 0)
    inside = valid[...]

    @pl.loop(0, MODES // 4)
    def _(block):
        pairs = [flipped[...] * flipped[pl.ds(block * 4 + k, 1), :] for k in range(4)]
        high, low = split(jnp.concatenate(pairs, axis=0))
        for part in range(COLS // 256):
            cols = slice(part * 256, (part + 1) * 256)
            held = weight[:, cols]
            sums = (dot(high, held) + dot(low, held)) * inside[:, cols]
            for k in range(4):
                ridge = jnp.where(eye_row[:, cols] == block * 4 + k, damping, 0.0)
                gram[block * 4 + k, :, cols] = sums[k * MODES : (k + 1) * MODES] + ridge

    @pl.loop(0, MODES)
    def _(k):
        scale = lax.rsqrt(gram[k, pl.ds(k, 1), :])
        column = jnp.where(eye_row >= k, gram[k] * scale, 0.0)
        gram[k] = column

        @pl.loop(k + 1, MODES)
        def _(j):
            gram[j] = gram[j] - gram[k] * gram[k, pl.ds(j, 1), :]

    def project(owner, out):
        pltpu.make_async_copy(got_mask.at[owner], got_mask.at[owner], mask_sem.at[owner]).wait()
        pltpu.make_async_copy(got_vis.at[owner], got_vis.at[owner], vis_sem.at[owner]).wait()

        @pl.loop(0, HALF // LANES)
        def _(group):
            narrow = pl.ds(pl.multiple_of(group * LANES, LANES), LANES)
            wide = pl.ds(pl.multiple_of(group * 2 * LANES, 2 * LANES), 2 * LANES)
            flags = jnp.concatenate([got_mask[owner, yy, :, narrow] for yy in range(NY)], axis=0)
            kept = widen((1 - flags).astype(F32))
            high, low = split(kept * got_vis[owner, :, wide])
            out[:, wide] = dot(chosen[...], jnp.concatenate([high, low, high], axis=0))

    def send(way, slot, rows):
        return pltpu.make_async_remote_copy(
            src_ref=partial.at[way, slot, rows],
            dst_ref=chain.at[way, slot, rows],
            send_sem=chain_send.at[way, slot],
            recv_sem=chain_sem.at[way, slot],
            device_id={"chan": at(y, ahead(1 - 2 * way), core)},
            device_id_type=MESH,
        )

    upper = pl.ds(0, MODES // 2)
    lower = pl.ds(MODES // 2, MODES // 2)
    project(ahead(4), partial.at[0, 0])
    partial[1, 0, MODES // 2 :] = partial[0, 0, MODES // 2 :]
    sends = [send(0, 0, upper), send(1, 0, lower)]
    for s in sends:
        s.start()
    everything = pl.ds(0, MODES)
    for slot in range(1, 4):
        for way in range(2):
            project(ahead((4 - slot) * (1 - 2 * way)), partial.at[way, slot])
            if slot == 1:
                piece = (upper, lower)[way]
                sends[way].wait_recv()
                partial[way, slot, piece] = partial[way, slot, piece] + chain[way, 0, piece]
            else:
                sends[(slot - 1) * 2 + way].wait_recv()
                partial[way, slot] = partial[way, slot] + chain[way, slot - 1]
            sends.append(send(way, slot, everything))
            sends[-1].start()
    project(z, answer)
    sends[6].wait_recv()
    sends[7].wait_recv()
    answer[...] = (answer[...] + chain[0, 3] + chain[1, 3]) * inside

    @pl.loop(0, MODES)
    def _(k):
        column = gram[k]
        row = answer[pl.ds(k, 1), :] / gram[k, pl.ds(k, 1), :]
        answer[...] = answer[...] - jnp.where(eye_row > k, column * row, 0.0)
        answer[pl.ds(k, 1), :] = row

    coef = coefs.at[y, z, core]
    coef[...] = jnp.zeros((MODES, COLS), F32)

    @pl.loop(0, MODES)
    def _(step):
        k = MODES - 1 - step
        later = jnp.sum(gram[k] * coef[...], axis=0, keepdims=True)
        coef[pl.ds(k, 1), :] = (answer[pl.ds(k, 1), :] - later) / gram[k, pl.ds(k, 1), :]

    pltpu.make_async_copy(kept_vis, kept_vis, load_sem.at[0]).wait()

    def push(piece, peer, arrived, sent=None):
        pltpu.make_async_remote_copy(
            src_ref=piece,
            dst_ref=piece,
            send_sem=link_send.at[0] if sent is None else sent,
            recv_sem=arrived,
            device_id={"chan": peer},
            device_id_type=MESH,
        ).start()

    def wait(piece, arrived):
        pltpu.make_async_copy(piece, piece, arrived).wait()

    def beside(way):
        return at(y, ahead(1 - 2 * way), core)

    def finish(yy, zz, cc, half):
        cols = (FIRST, SECOND)[half]
        block = at(yy, zz, cc)
        high, low = split(coefs[yy, zz, cc, :, cols])
        model = dot(basis[...], jnp.concatenate([high, low, high], axis=0))
        kept_vis[block, :, cols] = kept_vis[block, :, cols] - model
        start = pl.multiple_of(block * COLS + cols.start, LANES)
        pltpu.make_async_copy(
            kept_vis.at[block, :, cols], out.at[:, pl.ds(start, cols.stop - cols.start)], store_sem.at[0]
        ).start()

    def hand(half, yy, zz):
        cols = (FIRST, SECOND)[half]
        push(coefs.at[yy, zz, core, :, cols], at(y, z, 1 - core), twin_sem.at[half, yy, zz], twin_send.at[0])

    def take(half, yy, zz):
        wait(coefs.at[yy, zz, 1 - core, :, (FIRST, SECOND)[half]], twin_sem.at[half, yy, zz])
        finish(yy, zz, 1 - core, half)

    def along(yy, zz, way, far):
        if far < 4:
            push(coefs.at[yy, zz, core, :, FIRST], beside(way), along_sem.at[way, far, yy])
        elif far == 4:
            push(coefs.at[yy, zz, core, :, FIRST_OF[way]], beside(way), along_sem.at[way, far, yy])

    def first(zz, way, far):
        if far < 4:
            push(coefs.at[y, zz, core, :, SECOND], beside(way), first_sem.at[way, far])
        elif far == 4:
            push(coefs.at[y, zz, core, :, SECOND_OF[way]], beside(way), first_sem.at[way, far])

    def spread(zz):
        for step in (1, 3, 2):
            push(coefs.at[y, zz, core, :, SECOND], at((y + step) % NY, z, core), spread_sem.at[y, zz])

    for way in range(2):
        first(z, way, 1)
    for step in (1, 3, 2):
        push(coefs.at[y, z, core, :, FIRST], at((y + step) % NY, z, core), across_sem.at[y])
    for way in range(2):
        along(y, z, way, 1)
    spread(z)
    hand(0, y, z)
    hand(1, y, z)
    finish(y, z, core, 0)
    finish(y, z, core, 1)

    def origin(way, far):
        return ahead(far * (2 * way - 1))

    def second_of(far):
        if far == 4:
            zz = ahead(4)
            for way in range(2):
                wait(coefs.at[y, zz, core, :, SECOND_OF[way]], first_sem.at[way, 4])
            spread(zz)
            hand(1, y, zz)
            finish(y, zz, core, 1)
            return
        for way in range(2):
            zz = origin(way, far)
            wait(coefs.at[y, zz, core, :, SECOND], first_sem.at[way, far])
            first(zz, way, far + 1)
            spread(zz)
            hand(1, y, zz)
        for way in range(2):
            finish(y, origin(way, far), core, 1)

    def second_spread(far):
        @pl.loop(1, NY)
        def _(step):
            yy = (y + step) % NY
            for zz in (z,) if far == 0 else (ahead(4),) if far == 4 else (ahead(far), ahead(-far)):
                wait(coefs.at[yy, zz, core, :, SECOND], spread_sem.at[yy, zz])
                hand(1, yy, zz)
                finish(yy, zz, core, 1)

    def first_across():
        @pl.loop(1, NY)
        def _(step):
            yy = (y + step) % NY
            wait(coefs.at[yy, z, core, :, FIRST], across_sem.at[yy])
            for way in range(2):
                along(yy, z, way, 1)
            hand(0, yy, z)
            finish(yy, z, core, 0)

    def first_of(far):
        @pl.loop(0, NY)
        def _(step):
            yy = (y + step) % NY
            if far == 4:
                zz = ahead(4)
                for way in range(2):
                    wait(coefs.at[yy, zz, core, :, FIRST_OF[way]], along_sem.at[way, 4, yy])
                hand(0, yy, zz)
                finish(yy, zz, core, 0)
                return
            for way in range(2):
                zz = origin(way, far)
                wait(coefs.at[yy, zz, core, :, FIRST], along_sem.at[way, far, yy])
                along(yy, zz, way, far + 1)
                hand(0, yy, zz)
            for way in range(2):
                finish(yy, origin(way, far), core, 0)

    def taken(half, far):
        @pl.loop(0, NY)
        def _(step):
            yy = (y + step) % NY
            for zz in (z,) if far == 0 else (ahead(4),) if far == 4 else (ahead(far), ahead(-far)):
                take(half, yy, zz)

    second_of(1)
    first_across()
    second_spread(0)
    second_of(2)
    first_of(1)
    taken(0, 0)
    taken(1, 0)
    second_spread(1)
    second_of(3)
    first_of(2)
    taken(0, 1)
    taken(1, 1)
    second_spread(2)
    second_of(4)
    first_of(3)
    taken(0, 2)
    taken(1, 2)
    second_spread(3)
    first_of(4)
    second_spread(4)
    taken(0, 3)
    taken(1, 3)
    taken(0, 4)
    taken(1, 4)

    pltpu.make_async_copy(kept_vis, kept_vis, store_sem.at[0]).wait()
    pltpu.make_async_copy(gram.at[: MODES - 1], gram.at[: MODES - 1], link_send.at[0]).wait()
    pltpu.make_async_copy(gram, gram, twin_send.at[0]).wait()
    for s in sends:
        s.wait_send()
    sent = table.at[pl.ds(0, (NX - 1) * SLAB)]
    pltpu.make_async_copy(sent, sent, send_sem.at[0]).wait()
    sent = got_mask.at[pl.ds(0, NZ - 1)]
    pltpu.make_async_copy(sent, sent, send_sem.at[1]).wait()
    sent = got_vis.at[pl.ds(0, NY * NC - 1)]
    pltpu.make_async_copy(sent, sent, send_sem.at[2]).wait()


def fit(vis, mask, modes, valid):
    anywhere = pl.BlockSpec(memory_space=pl.ANY)
    held = pl.BlockSpec(memory_space=pltpu.VMEM)
    return pl.pallas_call(
        fit_kernel,
        out_shape=jax.ShapeDtypeStruct(vis.shape, F32),
        in_specs=[anywhere, anywhere, anywhere, held],
        out_specs=anywhere,
        scratch_shapes=[
            pltpu.VMEM((NY, NZ, NC, MODES, COLS), F32),
            pltpu.VMEM((ROWS, 3 * MODES), BF16),
            pltpu.VMEM((NY * NZ * NC, ROWS, COLS), F32),
            pltpu.VMEM((NX * SLAB, LANES), F32),
            pltpu.VMEM((NY, NZ, NC * ROWS, HALF), jnp.int32),
            pltpu.VMEM((NZ, NY, NC * ROWS, HALF), jnp.int32),
            pltpu.VMEM((NZ, SEL, COLS), F32),
            pltpu.VMEM((NX * SLAB, COLS), BF16),
            pltpu.VMEM((MODES, MODES, COLS), F32),
            pltpu.VMEM((MODES, NX * SLAB), F32),
            pltpu.VMEM((MODES, 3 * SEL), BF16),
            pltpu.VMEM((2, 4, MODES, COLS), F32),
            pltpu.VMEM((2, 4, MODES, COLS), F32),
            pltpu.VMEM((MODES, COLS), F32),
            pltpu.SemaphoreType.DMA((1,)),
            pltpu.SemaphoreType.DMA((2,)),
            pltpu.SemaphoreType.DMA((NZ,)),
            pltpu.SemaphoreType.DMA((NZ,)),
            pltpu.SemaphoreType.DMA((2, 4)),
            pltpu.SemaphoreType.DMA((3,)),
            pltpu.SemaphoreType.DMA((2, 4)),
            pltpu.SemaphoreType.DMA((NY,)),
            pltpu.SemaphoreType.DMA((2, 5, NY)),
            pltpu.SemaphoreType.DMA((2, 5)),
            pltpu.SemaphoreType.DMA((NY, NZ)),
            pltpu.SemaphoreType.DMA((2, NY, NZ)),
            pltpu.SemaphoreType.DMA((1,)),
            pltpu.SemaphoreType.DMA((1,)),
            pltpu.SemaphoreType.DMA((1,)),
            pltpu.SemaphoreType.DMA((1,)),
        ],
        compiler_params=pltpu.CompilerParams(
            collective_id=0, has_side_effects=True, vmem_limit_bytes=60 * 1024 * 1024
        ),
        name="fit",
    )(vis, mask, modes, valid)


def per_device(visibility, interference_mask, valid_time_count, fit_modes):
    owned = valid_time_count.shape[0]
    times = HALF // owned
    inside = lax.broadcasted_iota(jnp.int32, (owned, 2, times), 2) < valid_time_count[:, None, None]
    valid = inside.astype(F32).reshape(1, COLS)
    modes = jnp.pad(fit_modes, ((0, 0), (0, LANES - MODES)))
    mask = interference_mask.reshape(NY, NZ, NC * ROWS, HALF)
    return fit(visibility, mask, modes, valid)


def solution(mesh):
    placed = (P("chan", "grp"), P(None, ("grp", "chan")), P(("grp", "chan")), P("grp", None))
    return jax.shard_map(
        per_device, mesh=mesh, in_specs=placed, out_specs=P("chan", "grp"), check_vma=False
    )
```

```python
import functools

import jax
import jax.numpy as jnp
from jax import lax
from jax.experimental import pallas as pl
from jax.experimental.pallas import tpu as pltpu
from jax.sharding import PartitionSpec as P

MESH = pl.DeviceIdType.MESH
damping = 0.1

NX = 4
NY = 4
NZ = 8
NC = 2
MODES = 32
LANES = 128
ROWS = 16
SLAB = 256
TIMES = 32
COLS = 1024
HALF = 512
SEL = NY * NC * ROWS
SECOND, FIRST = slice(0, 768), slice(768, 1024)
TURNS = SECOND, FIRST
SECOND_OF = slice(0, 384), slice(384, 768)
F32 = jnp.float32
BF16 = jnp.bfloat16


def split(value):
    high = value.astype(BF16)
    low = (value - high.astype(F32)).astype(BF16)
    return high, low


def widen(mask):
    lane = lax.broadcasted_iota(jnp.int32, mask.shape, 1)
    by32 = pltpu.roll(mask, 32, 1)
    by64 = pltpu.roll(mask, 64, 1)
    by96 = pltpu.roll(mask, 96, 1)
    first = jnp.where(lane < 32, mask, jnp.where(lane < 96, by32, by64))
    second = jnp.where(lane < 32, by64, jnp.where(lane < 96, by96, mask))
    return jnp.concatenate([first, second], axis=1)


def dot(a, b):
    return lax.dot_general(a, b, (((1,), (0,)), ((), ())), preferred_element_type=F32)


def fit_kernel(
    vis,
    mask,
    modes,
    counts,
    out,
    valid,
    coefs,
    basis,
    kept_vis,
    table,
    got_mask,
    got_vis,
    weight,
    gram,
    flipped,
    chosen,
    partial,
    chain,
    answer,
    table_sem,
    mask_sem,
    vis_sem,
    chain_sem,
    send_sem,
    chain_send,
    across_sem,
    along_sem,
    first_sem,
    spread_sem,
    relay_sem,
    twin_sem,
    load_sem,
    link_send,
    twin_send,
):
    x = lax.axis_index("grp")
    chan = lax.axis_index("chan")
    y = chan // (NZ * NC)
    z = (chan // NC) % NZ
    core = chan % NC

    def at(yy, zz, cc):
        return (yy * NZ + zz) * NC + cc

    def ahead(steps):
        return (z + steps + NZ) % NZ

    barrier = pltpu.get_barrier_semaphore()
    for step in range(1, NX):
        pl.semaphore_signal(barrier, 1, device_id={"grp": (x + step) % NX}, device_id_type=MESH)
    for step in range(1, NZ):
        pl.semaphore_signal(barrier, 1, device_id={"chan": at(y, ahead(step), core)}, device_id_type=MESH)
    for step in range(1, NY * NC):
        peer = at((y + step // NC) % NY, z, (core + step) % NC)
        pl.semaphore_signal(barrier, 1, device_id={"chan": peer}, device_id_type=MESH)

    mine = y * NC + core
    flipped[:, pl.ds(pl.multiple_of(x * SLAB, SLAB), SLAB)] = modes[...]
    got_mask[z] = mask[:, z]
    for turn, cols in enumerate(TURNS):
        for zz in range(NZ):
            start = pl.multiple_of(at(y, zz, core) * COLS + cols.start, LANES)
            pltpu.make_async_copy(
                vis.at[:, pl.ds(start, cols.stop - cols.start)],
                got_vis.at[zz, pl.ds(pl.multiple_of(mine * ROWS, ROWS), ROWS), cols],
                vis_sem.at[turn, zz],
            ).start()

    pl.semaphore_wait(barrier, NX - 1 + NZ - 1 + NY * NC - 1)

    for step in range(1, NX):
        pltpu.make_async_remote_copy(
            src_ref=modes,
            dst_ref=flipped.at[:, pl.ds(pl.multiple_of(x * SLAB, SLAB), SLAB)],
            send_sem=send_sem.at[0],
            recv_sem=table_sem.at[0],
            device_id={"grp": (x + step) % NX},
            device_id_type=MESH,
        ).start()

    def send_mask(turn, *distances):
        cols = slice(TURNS[turn].start // 2, TURNS[turn].stop // 2)
        for steps in distances:
            there = ahead(steps)
            pltpu.make_async_remote_copy(
                src_ref=mask.at[:, there, :, cols],
                dst_ref=got_mask.at[z, :, :, cols],
                send_sem=send_sem.at[1],
                recv_sem=mask_sem.at[turn, z],
                device_id={"chan": at(y, there, core)},
                device_id_type=MESH,
            ).start()

    def send_vis():
        for turn, cols in enumerate(TURNS):
            for steps in (4, 3, -3, 2, -2, 1, -1, 0):
                owner = ahead(steps)
                for step in range(1, NY * NC):
                    yy = (y + step // NC) % NY
                    cc = (core + step) % NC
                    start = pl.multiple_of(at(yy, owner, cc) * COLS + cols.start, LANES)
                    pltpu.make_async_remote_copy(
                        src_ref=vis.at[:, pl.ds(start, cols.stop - cols.start)],
                        dst_ref=got_vis.at[owner, pl.ds(pl.multiple_of(mine * ROWS, ROWS), ROWS), cols],
                        send_sem=send_sem.at[2],
                        recv_sem=vis_sem.at[turn, owner],
                        device_id={"chan": at(yy, z, cc)},
                        device_id_type=MESH,
                    ).start()

        @pl.loop(0, NY * NZ * NC)
        def _(block):
            source = vis.at[:, pl.ds(pl.multiple_of(block * COLS, COLS), COLS)]
            pltpu.make_async_copy(source, kept_vis.at[block], load_sem.at[0]).start()

    eye_row = lax.broadcasted_iota(jnp.int32, (MODES, COLS), 0)

    def weigh():
        @pl.loop(0, NY * NZ)
        def _(block):
            yy = block // NZ
            zz = block % NZ
            for group in range(HALF // LANES):
                kept = 1 - mask[yy, zz, :, group * LANES : (group + 1) * LANES]
                weight[
                    pl.ds(pl.multiple_of(block * 32, 32), 32), group * 2 * LANES : (group + 1) * 2 * LANES
                ] = widen(kept.astype(F32)).astype(BF16)

        others = flipped.at[:, pl.ds(0, (NX - 1) * SLAB)]
        pltpu.make_async_copy(others, others, table_sem.at[0]).wait()
        filler = jnp.zeros((LANES - MODES, NX * SLAB), F32)
        table[...] = jnp.transpose(jnp.concatenate([flipped[...], filler], axis=0))
        rows = [
            table[pl.ds(pl.multiple_of(yy * SLAB + z * NC * ROWS, 32), NC * ROWS), :] for yy in range(NY)
        ]
        high, low = split(jnp.transpose(jnp.concatenate(rows, axis=0))[:MODES])
        chosen[...] = jnp.concatenate([high, high, low], axis=1)

        high, low = split(table[pl.ds(pl.multiple_of(chan * ROWS, ROWS), ROWS), :][:, :MODES])
        basis[...] = jnp.concatenate([high, high, low], axis=1)

    def make_gram():
        column = lax.broadcasted_iota(jnp.int32, (2 * LANES, COLS), 1)
        owner = lax.broadcasted_iota(jnp.int32, (2 * LANES, COLS), 0)
        picked = jnp.where(column // TIMES // 2 == owner, 1.0, 0.0).astype(BF16)
        filler = jnp.zeros((8, 2 * LANES - counts.shape[1]), F32)
        count = jnp.concatenate([jnp.broadcast_to(counts[...].astype(F32), (8, counts.shape[1])), filler], axis=1)
        count = dot(count.astype(BF16), picked)[:1]
        times = lax.broadcasted_iota(jnp.int32, (1, COLS), 1) % TIMES
        valid[...] = jnp.where(times.astype(F32) < count, 1.0, 0.0)
        inside = valid[...]

        @pl.loop(0, MODES // 4)
        def _(block):
            pairs = [flipped[...] * flipped[pl.ds(block * 4 + k, 1), :] for k in range(4)]
            high, low = split(jnp.concatenate(pairs, axis=0))
            for part in range(COLS // 256):
                cols = slice(part * 256, (part + 1) * 256)
                held = weight[:, cols]
                sums = (dot(high, held) + dot(low, held)) * inside[:, cols]
                for k in range(4):
                    ridge = jnp.where(eye_row[:, cols] == block * 4 + k, damping, 0.0)
                    gram[block * 4 + k, :, cols] = sums[k * MODES : (k + 1) * MODES] + ridge

    def factor():
        @pl.loop(0, MODES)
        def _(k):
            scale = lax.rsqrt(gram[k, pl.ds(k, 1), :])
            column = jnp.where(eye_row >= k, gram[k] * scale, 0.0)
            gram[k] = column

            @pl.loop(k + 1, MODES)
            def _(j):
                gram[j] = gram[j] - gram[k] * gram[k, pl.ds(j, 1), :]

    def project(turn, owner, out, own=False):
        cols = TURNS[turn]
        if not own:
            flags = got_mask.at[owner, :, :, slice(cols.start // 2, cols.stop // 2)]
            pltpu.make_async_copy(flags, flags, mask_sem.at[turn, owner]).wait()
        values = got_vis.at[owner, :, cols]
        pltpu.make_async_copy(values, values, vis_sem.at[turn, owner]).wait()

        @pl.loop(cols.start // (2 * LANES), cols.stop // (2 * LANES))
        def _(group):
            narrow = pl.ds(pl.multiple_of(group * LANES, LANES), LANES)
            wide = pl.ds(pl.multiple_of(group * 2 * LANES, 2 * LANES), 2 * LANES)
            flags = jnp.concatenate([got_mask[owner, yy, :, narrow] for yy in range(NY)], axis=0)
            kept = widen((1 - flags).astype(F32))
            high, low = split(kept * got_vis[owner, :, wide])
            out[:, wide] = dot(chosen[...], jnp.concatenate([high, low, high], axis=0))

    pieces = pl.ds(0, MODES // 2), pl.ds(MODES // 2, MODES // 2)
    sends = {}

    def send(turn, way, slot):
        piece = (way, slot, pieces[way] if slot == 0 else pl.ds(0, MODES), TURNS[turn])
        sends[turn, way, slot] = pltpu.make_async_remote_copy(
            src_ref=partial.at[piece],
            dst_ref=chain.at[piece],
            send_sem=chain_send.at[turn, way, slot],
            recv_sem=chain_sem.at[turn, way, slot],
            device_id={"chan": at(y, ahead(1 - 2 * way), core)},
            device_id_type=MESH,
        )
        sends[turn, way, slot].start()

    def begin(turn):
        cols = TURNS[turn]
        project(turn, ahead(4), partial.at[0, 0])
        partial[1, 0, MODES // 2 :, cols] = partial[0, 0, MODES // 2 :, cols]
        for way in range(2):
            send(turn, way, 0)

    def step_on(turn, slot):
        for way in range(2):
            project(turn, ahead((4 - slot) * (1 - 2 * way)), partial.at[way, slot])
            rows = pieces[way] if slot == 1 else pl.ds(0, MODES)
            cols = TURNS[turn]
            sends[turn, way, slot - 1].wait_recv()
            partial[way, slot, rows, cols] = partial[way, slot, rows, cols] + chain[way, slot - 1, rows, cols]
            send(turn, way, slot)

    def conclude(turn):
        cols = TURNS[turn]
        project(turn, z, answer, own=True)
        for way in range(2):
            sends[turn, way, 3].wait_recv()
        answer[:, cols] = (answer[:, cols] + chain[0, 3, :, cols] + chain[1, 3, :, cols]) * valid[:, cols]

        @pl.loop(0, MODES)
        def _(k):
            row = answer[pl.ds(k, 1), cols] / gram[k, pl.ds(k, 1), cols]
            answer[:, cols] = answer[:, cols] - jnp.where(eye_row[:, cols] > k, gram[k, :, cols] * row, 0.0)
            answer[pl.ds(k, 1), cols] = row

        coef = coefs.at[y, z, core]
        coef[:, cols] = jnp.zeros((MODES, cols.stop - cols.start), F32)

        @pl.loop(0, MODES)
        def _(step):
            k = MODES - 1 - step
            later = jnp.sum(gram[k, :, cols] * coef[:, cols], axis=0, keepdims=True)
            coef[pl.ds(k, 1), cols] = (answer[pl.ds(k, 1), cols] - later) / gram[k, pl.ds(k, 1), cols]


    def push(piece, peer, arrived, sent=None):
        pltpu.make_async_remote_copy(
            src_ref=piece,
            dst_ref=piece,
            send_sem=link_send.at[0] if sent is None else sent,
            recv_sem=arrived,
            device_id={"chan": peer},
            device_id_type=MESH,
        ).start()

    def wait(piece, arrived):
        pltpu.make_async_copy(piece, piece, arrived).wait()

    def beside(way):
        return at(y, ahead(1 - 2 * way), core)

    def finish(half, *places):
        cols = (FIRST, SECOND)[half]
        results = []
        for place in places:
            high, low = split(coefs[(*place, slice(None), cols)])
            model = dot(basis[...], jnp.concatenate([high, low, high], axis=0))
            results.append(kept_vis[at(*place), :, cols] - model)
        for place, result in zip(places, results):
            start = pl.multiple_of(at(*place) * COLS + cols.start, LANES)
            out[:, pl.ds(start, cols.stop - cols.start)] = result

    def hand(half, yy, zz):
        cols = (FIRST, SECOND)[half]
        push(coefs.at[yy, zz, core, :, cols], at(y, z, 1 - core), twin_sem.at[half, yy, zz], twin_send.at[0])

    def along(yy, zz, way, far):
        def go():
            push(coefs.at[yy, zz, core, :, FIRST], beside(way), along_sem.at[way, far, yy])

        if far < 4:
            go()
        elif far == 4:
            pl.when(yy % 2 == way)(go)

    def first(zz, way, far):
        if far < 4:
            push(coefs.at[y, zz, core, :, SECOND], beside(way), first_sem.at[way, far])
        elif far == 4:
            push(coefs.at[y, zz, core, :, SECOND_OF[way]], beside(way), first_sem.at[way, far])

    def above(way):
        return at((y + 1 - 2 * way + NY) % NY, z, core)

    def spread(zz):
        for way in range(2):
            push(coefs.at[y, zz, core, :, SECOND], above(way), spread_sem.at[way, zz])

    def start_second():
        pltpu.make_async_copy(kept_vis, kept_vis, load_sem.at[0]).wait()
        for way in range(2):
            first(z, way, 1)
        spread(z)
        hand(1, y, z)
        finish(1, (y, z, core))

    def start_first():
        for step in (1, 3, 2):
            push(coefs.at[y, z, core, :, FIRST], at((y + step) % NY, z, core), across_sem.at[y])
        for way in range(2):
            along(y, z, way, 1)
        hand(0, y, z)
        finish(0, (y, z, core))

    def origin(way, far):
        return ahead(far * (2 * way - 1))

    def second_of(far):
        if far == 4:
            zz = ahead(4)
            for way in range(2):
                wait(coefs.at[y, zz, core, :, SECOND_OF[way]], first_sem.at[way, 4])
            spread(zz)
            hand(1, y, zz)
            finish(1, (y, zz, core))
            return
        for way in range(2):
            zz = origin(way, far)
            wait(coefs.at[y, zz, core, :, SECOND], first_sem.at[way, far])
            first(zz, way, far + 1)
            spread(zz)
            hand(1, y, zz)
        finish(1, *[(y, origin(way, far), core) for way in range(2)])

    def near(far):
        return (z,) if far == 0 else (ahead(4),) if far == 4 else (ahead(far), ahead(-far))

    def second_spread(far):
        for zz in near(far):
            for way in range(2):
                yy = (y + 2 * way - 1 + NY) % NY
                wait(coefs.at[yy, zz, core, :, SECOND], spread_sem.at[way, zz])

                @pl.when(zz % 2 == way)
                def _():
                    push(coefs.at[yy, zz, core, :, SECOND], above(way), relay_sem.at[zz])

                hand(1, yy, zz)
        finish(1, *[((y + step) % NY, zz, core) for zz in near(far) for step in (1, 3)])

    def second_relay(far):
        yy = (y + 2) % NY
        for zz in near(far):
            wait(coefs.at[yy, zz, core, :, SECOND], relay_sem.at[zz])
            hand(1, yy, zz)
        finish(1, *[(yy, zz, core) for zz in near(far)])

    def first_across():
        @pl.loop(1, NY)
        def _(step):
            yy = (y + step) % NY
            wait(coefs.at[yy, z, core, :, FIRST], across_sem.at[yy])
            for way in range(2):
                along(yy, z, way, 1)
            hand(0, yy, z)

        finish(0, *[((y + step) % NY, z, core) for step in range(1, NY)])

    def first_of(far):
        @pl.loop(0, NY)
        def _(step):
            yy = (y + step) % NY
            if far == 4:
                zz = ahead(4)
                wait(coefs.at[yy, zz, core, :, FIRST], along_sem.at[yy % 2, 4, yy])
                hand(0, yy, zz)
                return
            for way in range(2):
                zz = origin(way, far)
                wait(coefs.at[yy, zz, core, :, FIRST], along_sem.at[way, far, yy])
                along(yy, zz, way, far + 1)
                hand(0, yy, zz)

        finish(0, *[(yy, zz, core) for yy in range(NY) for zz in near(far)])

    def taken(half, far):
        @pl.loop(0, NY)
        def _(yy):
            for zz in near(far):
                wait(coefs.at[yy, zz, 1 - core, :, (FIRST, SECOND)[half]], twin_sem.at[half, yy, zz])

        finish(half, *[(yy, zz, 1 - core) for yy in range(NY) for zz in near(far)])

    send_mask(0, 4, 3, -3)
    send_vis()
    weigh()
    make_gram()
    begin(0)
    send_mask(0, 2, -2)
    factor()
    step_on(0, 1)
    send_mask(0, 1, -1)
    send_mask(1, 4)
    step_on(0, 2)
    send_mask(1, 3, -3)
    begin(1)
    step_on(0, 3)
    send_mask(1, 2, -2)
    step_on(1, 1)
    send_mask(1, 1, -1)
    conclude(0)
    start_second()
    step_on(1, 2)
    second_of(1)
    step_on(1, 3)
    second_spread(0)
    second_of(2)
    conclude(1)
    start_first()
    second_spread(1)
    second_relay(0)
    first_across()
    second_of(3)
    taken(1, 0)
    first_of(1)
    second_spread(2)
    second_relay(1)
    second_of(4)
    first_of(2)
    taken(1, 1)
    second_spread(3)
    second_relay(2)
    first_of(3)
    taken(0, 0)
    taken(1, 2)
    second_spread(4)
    second_relay(3)
    first_of(4)
    taken(0, 1)
    taken(0, 2)
    second_relay(4)
    taken(1, 3)
    taken(0, 3)
    taken(0, 4)
    taken(1, 4)

    pltpu.make_async_copy(gram.at[: MODES - 1], gram.at[: MODES - 1], link_send.at[0]).wait()
    pltpu.make_async_copy(gram, gram, twin_send.at[0]).wait()
    for s in sends.values():
        s.wait_send()
    sent = flipped.at[:, pl.ds(0, (NX - 1) * SLAB)]
    pltpu.make_async_copy(sent, sent, send_sem.at[0]).wait()
    sent = got_mask.at[pl.ds(0, NZ - 1)]
    pltpu.make_async_copy(sent, sent, send_sem.at[1]).wait()
    sent = got_vis.at[pl.ds(0, NY * NC - 1)]
    pltpu.make_async_copy(sent, sent, send_sem.at[2]).wait()


def fit(vis, mask, modes, counts):
    outside = pl.BlockSpec(memory_space=pltpu.HBM)
    held = pl.BlockSpec(memory_space=pltpu.VMEM)
    return pl.pallas_call(
        fit_kernel,
        out_shape=jax.ShapeDtypeStruct(vis.shape, F32),
        in_specs=[outside, held, held, held],
        out_specs=held,
        scratch_shapes=[
            pltpu.VMEM((1, COLS), F32),
            pltpu.VMEM((NY, NZ, NC, MODES, COLS), F32),
            pltpu.VMEM((ROWS, 3 * MODES), BF16),
            pltpu.VMEM((NY * NZ * NC, ROWS, COLS), F32),
            pltpu.VMEM((NX * SLAB, LANES), F32),
            pltpu.VMEM((NZ, NY, NC * ROWS, HALF), jnp.int32),
            pltpu.VMEM((NZ, SEL, COLS), F32),
            pltpu.VMEM((NX * SLAB, COLS), BF16),
            pltpu.VMEM((MODES, MODES, COLS), F32),
            pltpu.VMEM((MODES, NX * SLAB), F32),
            pltpu.VMEM((MODES, 3 * SEL), BF16),
            pltpu.VMEM((2, 4, MODES, COLS), F32),
            pltpu.VMEM((2, 4, MODES, COLS), F32),
            pltpu.VMEM((MODES, COLS), F32),
            pltpu.SemaphoreType.DMA((1,)),
            pltpu.SemaphoreType.DMA((2, NZ)),
            pltpu.SemaphoreType.DMA((2, NZ)),
            pltpu.SemaphoreType.DMA((2, 2, 4)),
            pltpu.SemaphoreType.DMA((3,)),
            pltpu.SemaphoreType.DMA((2, 2, 4)),
            pltpu.SemaphoreType.DMA((NY,)),
            pltpu.SemaphoreType.DMA((2, 5, NY)),
            pltpu.SemaphoreType.DMA((2, 5)),
            pltpu.SemaphoreType.DMA((2, NZ)),
            pltpu.SemaphoreType.DMA((NZ,)),
            pltpu.SemaphoreType.DMA((2, NY, NZ)),
            pltpu.SemaphoreType.DMA((1,)),
            pltpu.SemaphoreType.DMA((1,)),
            pltpu.SemaphoreType.DMA((1,)),
        ],
        compiler_params=pltpu.CompilerParams(
            collective_id=0, has_side_effects=True, vmem_limit_bytes=44 * 1024 * 1024
        ),
        name="fit",
    )(vis, mask, modes, counts)


def per_device(visibility, interference_mask, valid_time_count, fit_modes):
    mask = interference_mask.reshape(NY, NZ, NC * ROWS, HALF)
    return fit(visibility, mask, fit_modes.T, valid_time_count.reshape(1, -1))


def solution(mesh):
    placed = (P("chan", "grp"), P(None, ("grp", "chan")), P(("grp", "chan")), P("grp", None))
    return jax.shard_map(
        per_device, mesh=mesh, in_specs=placed, out_specs=P("chan", "grp"), check_vma=False
    )
```

```python
import functools

import jax
import jax.numpy as jnp
from jax import lax
from jax.experimental import pallas as pl
from jax.experimental.pallas import tpu as pltpu
from jax.sharding import PartitionSpec as P

MESH = pl.DeviceIdType.MESH
damping = 0.1

NX = 4
NY = 4
NZ = 8
NC = 2
MODES = 32
LANES = 128
ROWS = 16
SLAB = 256
TIMES = 32
COLS = 1024
HALF = 512
SEL = NY * NC * ROWS
SECOND, FIRST = slice(0, 768), slice(768, 1024)
TURNS = SECOND, FIRST
SECOND_OF = slice(0, 384), slice(384, 768)
F32 = jnp.float32
BF16 = jnp.bfloat16


def split(value):
    high = value.astype(BF16)
    low = (value - high.astype(F32)).astype(BF16)
    return high, low


def widen(mask):
    lane = lax.broadcasted_iota(jnp.int32, mask.shape, 1)
    by32 = pltpu.roll(mask, 32, 1)
    by64 = pltpu.roll(mask, 64, 1)
    by96 = pltpu.roll(mask, 96, 1)
    first = jnp.where(lane < 32, mask, jnp.where(lane < 96, by32, by64))
    second = jnp.where(lane < 32, by64, jnp.where(lane < 96, by96, mask))
    return jnp.concatenate([first, second], axis=1)


def dot(a, b):
    return lax.dot_general(a, b, (((1,), (0,)), ((), ())), preferred_element_type=F32)


def fit_kernel(
    vis,
    mask,
    modes,
    counts,
    out,
    valid,
    coefs,
    basis,
    kept_vis,
    table,
    got_mask,
    got_vis,
    weight,
    gram,
    flipped,
    chosen,
    partial,
    chain,
    answer,
    table_sem,
    mask_sem,
    vis_sem,
    chain_sem,
    send_sem,
    chain_send,
    across_sem,
    along_sem,
    first_sem,
    spread_sem,
    relay_sem,
    twin_sem,
    load_sem,
    link_send,
    twin_send,
):
    x = lax.axis_index("grp")
    chan = lax.axis_index("chan")
    y = chan // (NZ * NC)
    z = (chan // NC) % NZ
    core = chan % NC

    def at(yy, zz, cc):
        return (yy * NZ + zz) * NC + cc

    def ahead(steps):
        return (z + steps + NZ) % NZ

    barrier = pltpu.get_barrier_semaphore()
    for step in range(1, NX):
        pl.semaphore_signal(barrier, 1, device_id={"grp": (x + step) % NX}, device_id_type=MESH)
    for step in range(1, NZ):
        pl.semaphore_signal(barrier, 1, device_id={"chan": at(y, ahead(step), core)}, device_id_type=MESH)
    for step in range(1, NY * NC):
        peer = at((y + step // NC) % NY, z, (core + step) % NC)
        pl.semaphore_signal(barrier, 1, device_id={"chan": peer}, device_id_type=MESH)

    mine = y * NC + core
    flipped[:, pl.ds(pl.multiple_of(x * SLAB, SLAB), SLAB)] = modes[...]
    got_mask[z] = mask[:, z]
    for turn, cols in enumerate(TURNS):
        for zz in range(NZ):
            start = pl.multiple_of(at(y, zz, core) * COLS + cols.start, LANES)
            pltpu.make_async_copy(
                vis.at[:, pl.ds(start, cols.stop - cols.start)],
                got_vis.at[zz, pl.ds(pl.multiple_of(mine * ROWS, ROWS), ROWS), cols],
                vis_sem.at[turn, zz],
            ).start()

    pl.semaphore_wait(barrier, NX - 1 + NZ - 1 + NY * NC - 1)

    for step in range(1, NX):
        pltpu.make_async_remote_copy(
            src_ref=modes,
            dst_ref=flipped.at[:, pl.ds(pl.multiple_of(x * SLAB, SLAB), SLAB)],
            send_sem=send_sem.at[0],
            recv_sem=table_sem.at[0],
            device_id={"grp": (x + step) % NX},
            device_id_type=MESH,
        ).start()

    def send_mask(turn, *distances):
        cols = slice(TURNS[turn].start // 2, TURNS[turn].stop // 2)
        for steps in distances:
            there = ahead(steps)
            pltpu.make_async_remote_copy(
                src_ref=mask.at[:, there, :, cols],
                dst_ref=got_mask.at[z, :, :, cols],
                send_sem=send_sem.at[1],
                recv_sem=mask_sem.at[turn, z],
                device_id={"chan": at(y, there, core)},
                device_id_type=MESH,
            ).start()

    def send_vis():
        for turn, cols in enumerate(TURNS):
            for steps in (4, 3, -3, 2, -2, 1, -1, 0):
                owner = ahead(steps)
                for step in range(1, NY * NC):
                    yy = (y + step // NC) % NY
                    cc = (core + step) % NC
                    start = pl.multiple_of(at(yy, owner, cc) * COLS + cols.start, LANES)
                    pltpu.make_async_remote_copy(
                        src_ref=vis.at[:, pl.ds(start, cols.stop - cols.start)],
                        dst_ref=got_vis.at[owner, pl.ds(pl.multiple_of(mine * ROWS, ROWS), ROWS), cols],
                        send_sem=send_sem.at[2],
                        recv_sem=vis_sem.at[turn, owner],
                        device_id={"chan": at(yy, z, cc)},
                        device_id_type=MESH,
                    ).start()

        @pl.loop(0, NY * NZ * NC)
        def _(block):
            source = vis.at[:, pl.ds(pl.multiple_of(block * COLS, COLS), COLS)]
            pltpu.make_async_copy(source, kept_vis.at[block], load_sem.at[0]).start()

    eye_row = lax.broadcasted_iota(jnp.int32, (MODES, COLS), 0)

    def weigh():
        @pl.loop(0, NY * NZ)
        def _(block):
            yy = block // NZ
            zz = block % NZ
            for group in range(HALF // LANES):
                kept = 1 - mask[yy, zz, :, group * LANES : (group + 1) * LANES]
                weight[
                    pl.ds(pl.multiple_of(block * 32, 32), 32), group * 2 * LANES : (group + 1) * 2 * LANES
                ] = widen(kept.astype(F32)).astype(BF16)

        others = flipped.at[:, pl.ds(0, (NX - 1) * SLAB)]
        pltpu.make_async_copy(others, others, table_sem.at[0]).wait()
        filler = jnp.zeros((LANES - MODES, NX * SLAB), F32)
        table[...] = jnp.transpose(jnp.concatenate([flipped[...], filler], axis=0))
        rows = [
            table[pl.ds(pl.multiple_of(yy * SLAB + z * NC * ROWS, 32), NC * ROWS), :] for yy in range(NY)
        ]
        high, low = split(jnp.transpose(jnp.concatenate(rows, axis=0))[:MODES])
        chosen[...] = jnp.concatenate([high, high, low], axis=1)

        high, low = split(table[pl.ds(pl.multiple_of(chan * ROWS, ROWS), ROWS), :][:, :MODES])
        basis[...] = jnp.concatenate([high, high, low], axis=1)

    def make_gram():
        column = lax.broadcasted_iota(jnp.int32, (2 * LANES, COLS), 1)
        owner = lax.broadcasted_iota(jnp.int32, (2 * LANES, COLS), 0)
        picked = jnp.where(column // TIMES // 2 == owner, 1.0, 0.0).astype(BF16)
        filler = jnp.zeros((8, 2 * LANES - counts.shape[1]), F32)
        count = jnp.concatenate([jnp.broadcast_to(counts[...].astype(F32), (8, counts.shape[1])), filler], axis=1)
        count = dot(count.astype(BF16), picked)[:1]
        times = lax.broadcasted_iota(jnp.int32, (1, COLS), 1) % TIMES
        valid[...] = jnp.where(times.astype(F32) < count, 1.0, 0.0)
        inside = valid[...]

        @pl.loop(0, MODES // 4)
        def _(block):
            pairs = [flipped[...] * flipped[pl.ds(block * 4 + k, 1), :] for k in range(4)]
            high, low = split(jnp.concatenate(pairs, axis=0))
            for part in range(COLS // 256):
                cols = slice(part * 256, (part + 1) * 256)
                held = weight[:, cols]
                sums = (dot(high, held) + dot(low, held)) * inside[:, cols]
                for k in range(4):
                    ridge = jnp.where(eye_row[:, cols] == block * 4 + k, damping, 0.0)
                    gram[block * 4 + k, :, cols] = sums[k * MODES : (k + 1) * MODES] + ridge

    def factor():
        @pl.loop(0, MODES)
        def _(k):
            scale = lax.rsqrt(gram[k, pl.ds(k, 1), :])
            column = jnp.where(eye_row >= k, gram[k] * scale, 0.0)
            gram[k] = column

            @pl.loop(k + 1, MODES)
            def _(j):
                gram[j] = gram[j] - gram[k] * gram[k, pl.ds(j, 1), :]

    def project(turn, owner, out, own=False):
        cols = TURNS[turn]
        if not own:
            flags = got_mask.at[owner, :, :, slice(cols.start // 2, cols.stop // 2)]
            pltpu.make_async_copy(flags, flags, mask_sem.at[turn, owner]).wait()
        values = got_vis.at[owner, :, cols]
        pltpu.make_async_copy(values, values, vis_sem.at[turn, owner]).wait()

        @pl.loop(cols.start // (2 * LANES), cols.stop // (2 * LANES))
        def _(group):
            narrow = pl.ds(pl.multiple_of(group * LANES, LANES), LANES)
            wide = pl.ds(pl.multiple_of(group * 2 * LANES, 2 * LANES), 2 * LANES)
            flags = jnp.concatenate([got_mask[owner, yy, :, narrow] for yy in range(NY)], axis=0)
            kept = widen((1 - flags).astype(F32))
            high, low = split(kept * got_vis[owner, :, wide])
            out[:, wide] = dot(chosen[...], jnp.concatenate([high, low, high], axis=0))

    pieces = pl.ds(0, MODES // 2), pl.ds(MODES // 2, MODES // 2)
    sends = {}

    def send(turn, way, slot):
        piece = (way, slot, pieces[way] if slot == 0 else pl.ds(0, MODES), TURNS[turn])
        sends[turn, way, slot] = pltpu.make_async_remote_copy(
            src_ref=partial.at[piece],
            dst_ref=chain.at[piece],
            send_sem=chain_send.at[turn, way, slot],
            recv_sem=chain_sem.at[turn, way, slot],
            device_id={"chan": at(y, ahead(1 - 2 * way), core)},
            device_id_type=MESH,
        )
        sends[turn, way, slot].start()

    def begin(turn):
        cols = TURNS[turn]
        project(turn, ahead(4), partial.at[0, 0])
        partial[1, 0, MODES // 2 :, cols] = partial[0, 0, MODES // 2 :, cols]
        for way in range(2):
            send(turn, way, 0)

    def step_on(turn, slot):
        for way in range(2):
            project(turn, ahead((4 - slot) * (1 - 2 * way)), partial.at[way, slot])
            rows = pieces[way] if slot == 1 else pl.ds(0, MODES)
            cols = TURNS[turn]
            sends[turn, way, slot - 1].wait_recv()
            partial[way, slot, rows, cols] = partial[way, slot, rows, cols] + chain[way, slot - 1, rows, cols]
            send(turn, way, slot)

    def conclude(turn):
        cols = TURNS[turn]
        project(turn, z, answer, own=True)
        for way in range(2):
            sends[turn, way, 3].wait_recv()
        answer[:, cols] = (answer[:, cols] + chain[0, 3, :, cols] + chain[1, 3, :, cols]) * valid[:, cols]

        @pl.loop(0, MODES)
        def _(k):
            row = answer[pl.ds(k, 1), cols] / gram[k, pl.ds(k, 1), cols]
            answer[:, cols] = answer[:, cols] - jnp.where(eye_row[:, cols] > k, gram[k, :, cols] * row, 0.0)
            answer[pl.ds(k, 1), cols] = row

        coef = coefs.at[y, z, core]
        coef[:, cols] = jnp.zeros((MODES, cols.stop - cols.start), F32)

        @pl.loop(0, MODES)
        def _(step):
            k = MODES - 1 - step
            later = jnp.sum(gram[k, :, cols] * coef[:, cols], axis=0, keepdims=True)
            coef[pl.ds(k, 1), cols] = (answer[pl.ds(k, 1), cols] - later) / gram[k, pl.ds(k, 1), cols]


    def push(piece, peer, arrived, sent=None):
        pltpu.make_async_remote_copy(
            src_ref=piece,
            dst_ref=piece,
            send_sem=link_send.at[0] if sent is None else sent,
            recv_sem=arrived,
            device_id={"chan": peer},
            device_id_type=MESH,
        ).start()

    def wait(piece, arrived):
        pltpu.make_async_copy(piece, piece, arrived).wait()

    def beside(way):
        return at(y, ahead(1 - 2 * way), core)

    def finish(half, *places):
        cols = (FIRST, SECOND)[half]
        results = []
        for place in places:
            high, low = split(coefs[(*place, slice(None), cols)])
            model = dot(basis[...], jnp.concatenate([high, low, high], axis=0))
            results.append(kept_vis[at(*place), :, cols] - model)
        for place, result in zip(places, results):
            start = pl.multiple_of(at(*place) * COLS + cols.start, LANES)
            out[:, pl.ds(start, cols.stop - cols.start)] = result

    def hand(half, yy, zz, far):
        cols = (FIRST, SECOND)[half]
        push(coefs.at[yy, zz, core, :, cols], at(y, z, 1 - core), twin_sem.at[half, far], twin_send.at[0])

    def along(yy, zz, way, far):
        def go():
            push(coefs.at[yy, zz, core, :, FIRST], beside(way), along_sem.at[way, far, yy])

        if far < 4:
            go()
        elif far == 4:
            pl.when(yy % 2 == way)(go)

    def first(zz, way, far):
        if far < 4:
            push(coefs.at[y, zz, core, :, SECOND], beside(way), first_sem.at[way, far])
        elif far == 4:
            push(coefs.at[y, zz, core, :, SECOND_OF[way]], beside(way), first_sem.at[way, far])

    def above(way):
        return at((y + 1 - 2 * way + NY) % NY, z, core)

    def spread(zz):
        for way in range(2):
            push(coefs.at[y, zz, core, :, SECOND], above(way), spread_sem.at[way, zz])

    def start_second():
        pltpu.make_async_copy(kept_vis, kept_vis, load_sem.at[0]).wait()
        for way in range(2):
            first(z, way, 1)
        spread(z)
        hand(1, y, z, 0)
        finish(1, (y, z, core))

    def start_first():
        for step in (1, 3, 2):
            push(coefs.at[y, z, core, :, FIRST], at((y + step) % NY, z, core), across_sem.at[y])
        for way in range(2):
            along(y, z, way, 1)
        hand(0, y, z, 0)
        finish(0, (y, z, core))

    def origin(way, far):
        return ahead(far * (2 * way - 1))

    def second_of(far):
        if far == 4:
            zz = ahead(4)
            for way in range(2):
                wait(coefs.at[y, zz, core, :, SECOND_OF[way]], first_sem.at[way, 4])
            spread(zz)
            hand(1, y, zz, far)
            finish(1, (y, zz, core))
            return
        for way in range(2):
            zz = origin(way, far)
            wait(coefs.at[y, zz, core, :, SECOND], first_sem.at[way, far])
            first(zz, way, far + 1)
            spread(zz)
            hand(1, y, zz, far)
        finish(1, *[(y, origin(way, far), core) for way in range(2)])

    def near(far):
        return (z,) if far == 0 else (ahead(4),) if far == 4 else (ahead(far), ahead(-far))

    def second_spread(far):
        for side, zz in enumerate(near(far)):
            for way in range(2):
                yy = (y + 2 * way - 1 + NY) % NY
                wait(coefs.at[yy, zz, core, :, SECOND], spread_sem.at[way, zz])

                def relay():
                    push(coefs.at[yy, zz, core, :, SECOND], above(way), relay_sem.at[zz])

                if far in (0, 4):
                    pl.when(yy % 2 == way)(relay)
                elif side == way:
                    relay()
                hand(1, yy, zz, far)
        finish(1, *[((y + step) % NY, zz, core) for zz in near(far) for step in (1, 3)])

    def second_relay(far):
        yy = (y + 2) % NY
        for zz in near(far):
            wait(coefs.at[yy, zz, core, :, SECOND], relay_sem.at[zz])
            hand(1, yy, zz, far)
        finish(1, *[(yy, zz, core) for zz in near(far)])

    def first_across():
        @pl.loop(1, NY)
        def _(step):
            yy = (y + step) % NY
            wait(coefs.at[yy, z, core, :, FIRST], across_sem.at[yy])
            for way in range(2):
                along(yy, z, way, 1)
            hand(0, yy, z, 0)

        finish(0, *[((y + step) % NY, z, core) for step in range(1, NY)])

    def first_of(far):
        @pl.loop(0, NY)
        def _(step):
            yy = (y + step) % NY
            if far == 4:
                zz = ahead(4)
                wait(coefs.at[yy, zz, core, :, FIRST], along_sem.at[yy % 2, 4, yy])
                hand(0, yy, zz, far)
                return
            for way in range(2):
                zz = origin(way, far)
                wait(coefs.at[yy, zz, core, :, FIRST], along_sem.at[way, far, yy])
                along(yy, zz, way, far + 1)
                hand(0, yy, zz, far)

        finish(0, *[(yy, zz, core) for yy in range(NY) for zz in near(far)])

    def taken(half, far):
        amount = coefs.at[:, : len(near(far)), 0, :, (FIRST, SECOND)[half]]
        wait(amount, twin_sem.at[half, far])
        finish(half, *[(yy, zz, 1 - core) for yy in range(NY) for zz in near(far)])

    send_mask(0, 4, 3, -3)
    send_vis()
    weigh()
    make_gram()
    begin(0)
    send_mask(0, 2, -2)
    factor()
    step_on(0, 1)
    send_mask(0, 1, -1)
    send_mask(1, 4)
    step_on(0, 2)
    send_mask(1, 3, -3)
    begin(1)
    step_on(0, 3)
    send_mask(1, 2, -2)
    step_on(1, 1)
    send_mask(1, 1, -1)
    conclude(0)
    start_second()
    step_on(1, 2)
    second_of(1)
    step_on(1, 3)
    second_spread(0)
    conclude(1)
    start_first()
    second_of(2)
    second_spread(1)
    second_relay(0)
    first_across()
    second_of(3)
    second_spread(2)
    first_of(1)
    second_relay(1)
    second_of(4)
    first_of(2)
    second_spread(3)
    second_relay(2)
    first_of(3)
    taken(1, 0)
    second_spread(4)
    taken(1, 1)
    first_of(4)
    taken(0, 0)
    taken(0, 1)
    second_relay(3)
    taken(1, 2)
    taken(0, 2)
    second_relay(4)
    taken(0, 3)
    taken(1, 3)
    taken(0, 4)
    taken(1, 4)

    pltpu.make_async_copy(gram.at[: MODES - 1], gram.at[: MODES - 1], link_send.at[0]).wait()
    pltpu.make_async_copy(gram, gram, twin_send.at[0]).wait()
    for s in sends.values():
        s.wait_send()
    sent = flipped.at[:, pl.ds(0, (NX - 1) * SLAB)]
    pltpu.make_async_copy(sent, sent, send_sem.at[0]).wait()
    sent = got_mask.at[pl.ds(0, NZ - 1)]
    pltpu.make_async_copy(sent, sent, send_sem.at[1]).wait()
    sent = got_vis.at[pl.ds(0, NY * NC - 1)]
    pltpu.make_async_copy(sent, sent, send_sem.at[2]).wait()


def fit(vis, mask, modes, counts):
    outside = pl.BlockSpec(memory_space=pltpu.HBM)
    held = pl.BlockSpec(memory_space=pltpu.VMEM)
    return pl.pallas_call(
        fit_kernel,
        out_shape=jax.ShapeDtypeStruct(vis.shape, F32),
        in_specs=[outside, held, held, held],
        out_specs=held,
        scratch_shapes=[
            pltpu.VMEM((1, COLS), F32),
            pltpu.VMEM((NY, NZ, NC, MODES, COLS), F32),
            pltpu.VMEM((ROWS, 3 * MODES), BF16),
            pltpu.VMEM((NY * NZ * NC, ROWS, COLS), F32),
            pltpu.VMEM((NX * SLAB, LANES), F32),
            pltpu.VMEM((NZ, NY, NC * ROWS, HALF), jnp.int32),
            pltpu.VMEM((NZ, SEL, COLS), F32),
            pltpu.VMEM((NX * SLAB, COLS), BF16),
            pltpu.VMEM((MODES, MODES, COLS), F32),
            pltpu.VMEM((MODES, NX * SLAB), F32),
            pltpu.VMEM((MODES, 3 * SEL), BF16),
            pltpu.VMEM((2, 4, MODES, COLS), F32),
            pltpu.VMEM((2, 4, MODES, COLS), F32),
            pltpu.VMEM((MODES, COLS), F32),
            pltpu.SemaphoreType.DMA((1,)),
            pltpu.SemaphoreType.DMA((2, NZ)),
            pltpu.SemaphoreType.DMA((2, NZ)),
            pltpu.SemaphoreType.DMA((2, 2, 4)),
            pltpu.SemaphoreType.DMA((3,)),
            pltpu.SemaphoreType.DMA((2, 2, 4)),
            pltpu.SemaphoreType.DMA((NY,)),
            pltpu.SemaphoreType.DMA((2, 5, NY)),
            pltpu.SemaphoreType.DMA((2, 5)),
            pltpu.SemaphoreType.DMA((2, NZ)),
            pltpu.SemaphoreType.DMA((NZ,)),
            pltpu.SemaphoreType.DMA((2, 5)),
            pltpu.SemaphoreType.DMA((1,)),
            pltpu.SemaphoreType.DMA((1,)),
            pltpu.SemaphoreType.DMA((1,)),
        ],
        compiler_params=pltpu.CompilerParams(
            collective_id=0, has_side_effects=True, vmem_limit_bytes=44 * 1024 * 1024
        ),
        name="fit",
    )(vis, mask, modes, counts)


def per_device(visibility, interference_mask, valid_time_count, fit_modes):
    mask = interference_mask.reshape(NY, NZ, NC * ROWS, HALF)
    return fit(visibility, mask, fit_modes.T, valid_time_count.reshape(1, -1))


def solution(mesh):
    placed = (P("chan", "grp"), P(None, ("grp", "chan")), P(("grp", "chan")), P("grp", None))
    return jax.shard_map(
        per_device, mesh=mesh, in_specs=placed, out_specs=P("chan", "grp"), check_vma=False
    )
```

```python
import functools

import jax
import jax.numpy as jnp
from jax import lax
from jax.experimental import pallas as pl
from jax.experimental.pallas import tpu as pltpu
from jax.sharding import PartitionSpec as P

MESH = pl.DeviceIdType.MESH
damping = 0.1

NX = 4
NY = 4
NZ = 8
NC = 2
MODES = 32
LANES = 128
ROWS = 16
SLAB = 256
TIMES = 32
COLS = 1024
HALF = 512
SEL = NY * NC * ROWS
SECOND, FIRST = slice(0, 768), slice(768, 1024)
TURNS = SECOND, FIRST
SECOND_OF = slice(0, 384), slice(384, 768)
F32 = jnp.float32
BF16 = jnp.bfloat16


def split(value):
    high = value.astype(BF16)
    low = (value - high.astype(F32)).astype(BF16)
    return high, low


def widen(mask):
    lane = lax.broadcasted_iota(jnp.int32, mask.shape, 1)
    by32 = pltpu.roll(mask, 32, 1)
    by64 = pltpu.roll(mask, 64, 1)
    by96 = pltpu.roll(mask, 96, 1)
    first = jnp.where(lane < 32, mask, jnp.where(lane < 96, by32, by64))
    second = jnp.where(lane < 32, by64, jnp.where(lane < 96, by96, mask))
    return jnp.concatenate([first, second], axis=1)


def dot(a, b):
    return lax.dot_general(a, b, (((1,), (0,)), ((), ())), preferred_element_type=F32)


def fit_kernel(
    vis,
    mask,
    modes,
    counts,
    out,
    inverse,
    valid,
    coefs,
    basis,
    kept_vis,
    table,
    got_mask,
    got_vis,
    weight,
    gram,
    flipped,
    chosen,
    partial,
    chain,
    answer,
    table_sem,
    mask_sem,
    vis_sem,
    chain_sem,
    send_sem,
    chain_send,
    across_sem,
    along_sem,
    first_sem,
    spread_sem,
    relay_sem,
    twin_sem,
    load_sem,
    link_send,
    twin_send,
):
    x = lax.axis_index("grp")
    chan = lax.axis_index("chan")
    y = chan // (NZ * NC)
    z = (chan // NC) % NZ
    core = chan % NC

    def at(yy, zz, cc):
        return (yy * NZ + zz) * NC + cc

    def ahead(steps):
        return (z + steps + NZ) % NZ

    barrier = pltpu.get_barrier_semaphore()
    for step in range(1, NX):
        pl.semaphore_signal(barrier, 1, device_id={"grp": (x + step) % NX}, device_id_type=MESH)
    for step in range(1, NZ):
        pl.semaphore_signal(barrier, 1, device_id={"chan": at(y, ahead(step), core)}, device_id_type=MESH)
    for step in range(1, NY * NC):
        peer = at((y + step // NC) % NY, z, (core + step) % NC)
        pl.semaphore_signal(barrier, 1, device_id={"chan": peer}, device_id_type=MESH)

    mine = y * NC + core
    flipped[:, pl.ds(pl.multiple_of(x * SLAB, SLAB), SLAB)] = modes[...]
    got_mask[z] = mask[:, z]
    for turn, cols in enumerate(TURNS):
        for zz in range(NZ):
            start = pl.multiple_of(at(y, zz, core) * COLS + cols.start, LANES)
            pltpu.make_async_copy(
                vis.at[:, pl.ds(start, cols.stop - cols.start)],
                got_vis.at[zz, pl.ds(pl.multiple_of(mine * ROWS, ROWS), ROWS), cols],
                vis_sem.at[turn, zz],
            ).start()

    pl.semaphore_wait(barrier, NX - 1 + NZ - 1 + NY * NC - 1)

    for step in range(1, NX):
        pltpu.make_async_remote_copy(
            src_ref=modes,
            dst_ref=flipped.at[:, pl.ds(pl.multiple_of(x * SLAB, SLAB), SLAB)],
            send_sem=send_sem.at[0],
            recv_sem=table_sem.at[0],
            device_id={"grp": (x + step) % NX},
            device_id_type=MESH,
        ).start()

    def send_mask(turn, *distances):
        cols = slice(TURNS[turn].start // 2, TURNS[turn].stop // 2)
        for steps in distances:
            there = ahead(steps)
            pltpu.make_async_remote_copy(
                src_ref=mask.at[:, there, :, cols],
                dst_ref=got_mask.at[z, :, :, cols],
                send_sem=send_sem.at[1],
                recv_sem=mask_sem.at[turn, z],
                device_id={"chan": at(y, there, core)},
                device_id_type=MESH,
            ).start()

    def send_vis():
        for turn, cols in enumerate(TURNS):
            for steps in (4, 3, -3, 2, -2, 1, -1, 0):
                owner = ahead(steps)
                for step in range(1, NY * NC):
                    yy = (y + step // NC) % NY
                    cc = (core + step) % NC
                    start = pl.multiple_of(at(yy, owner, cc) * COLS + cols.start, LANES)
                    pltpu.make_async_remote_copy(
                        src_ref=vis.at[:, pl.ds(start, cols.stop - cols.start)],
                        dst_ref=got_vis.at[owner, pl.ds(pl.multiple_of(mine * ROWS, ROWS), ROWS), cols],
                        send_sem=send_sem.at[2],
                        recv_sem=vis_sem.at[turn, owner],
                        device_id={"chan": at(yy, z, cc)},
                        device_id_type=MESH,
                    ).start()

        @pl.loop(0, NY * NZ * NC)
        def _(block):
            source = vis.at[:, pl.ds(pl.multiple_of(block * COLS, COLS), COLS)]
            pltpu.make_async_copy(source, kept_vis.at[block], load_sem.at[0]).start()

    eye_row = lax.broadcasted_iota(jnp.int32, (MODES, COLS), 0)

    def weigh():
        @pl.loop(0, NY * NZ)
        def _(block):
            yy = block // NZ
            zz = block % NZ
            for group in range(HALF // LANES):
                kept = 1 - mask[yy, zz, :, group * LANES : (group + 1) * LANES]
                weight[
                    pl.ds(pl.multiple_of(block * 32, 32), 32), group * 2 * LANES : (group + 1) * 2 * LANES
                ] = widen(kept.astype(F32)).astype(BF16)

        others = flipped.at[:, pl.ds(0, (NX - 1) * SLAB)]
        pltpu.make_async_copy(others, others, table_sem.at[0]).wait()
        filler = jnp.zeros((LANES - MODES, NX * SLAB), F32)
        table[...] = jnp.transpose(jnp.concatenate([flipped[...], filler], axis=0))
        rows = [
            table[pl.ds(pl.multiple_of(yy * SLAB + z * NC * ROWS, 32), NC * ROWS), :] for yy in range(NY)
        ]
        high, low = split(jnp.transpose(jnp.concatenate(rows, axis=0))[:MODES])
        chosen[...] = jnp.concatenate([high, high, low], axis=1)

        high, low = split(table[pl.ds(pl.multiple_of(chan * ROWS, ROWS), ROWS), :][:, :MODES])
        basis[...] = jnp.concatenate([high, high, low], axis=1)

    def make_gram():
        column = lax.broadcasted_iota(jnp.int32, (2 * LANES, COLS), 1)
        owner = lax.broadcasted_iota(jnp.int32, (2 * LANES, COLS), 0)
        picked = jnp.where(column // TIMES // 2 == owner, 1.0, 0.0).astype(BF16)
        filler = jnp.zeros((8, 2 * LANES - counts.shape[1]), F32)
        count = jnp.concatenate([jnp.broadcast_to(counts[...].astype(F32), (8, counts.shape[1])), filler], axis=1)
        count = dot(count.astype(BF16), picked)[:1]
        times = lax.broadcasted_iota(jnp.int32, (1, COLS), 1) % TIMES
        valid[...] = jnp.where(times.astype(F32) < count, 1.0, 0.0)
        inside = valid[...]

        @pl.loop(0, MODES // 4)
        def _(block):
            pairs = [flipped[...] * flipped[pl.ds(block * 4 + k, 1), :] for k in range(4)]
            high, low = split(jnp.concatenate(pairs, axis=0))
            for part in range(COLS // 256):
                cols = slice(part * 256, (part + 1) * 256)
                held = weight[:, cols]
                sums = (dot(high, held) + dot(low, held)) * inside[:, cols]
                for k in range(4):
                    ridge = jnp.where(eye_row[:, cols] == block * 4 + k, damping, 0.0)
                    gram[block * 4 + k, :, cols] = sums[k * MODES : (k + 1) * MODES] + ridge

    def factor():
        @pl.loop(0, MODES)
        def _(k):
            scale = lax.rsqrt(gram[k, pl.ds(k, 1), :])
            inverse[pl.ds(k, 1), :] = scale
            column = jnp.where(eye_row >= k, gram[k] * scale, 0.0)
            gram[k] = column

            @pl.loop(k + 1, MODES)
            def _(j):
                gram[j] = gram[j] - gram[k] * gram[k, pl.ds(j, 1), :]

    def project(turn, owner, out, own=False):
        cols = TURNS[turn]
        if not own:
            flags = got_mask.at[owner, :, :, slice(cols.start // 2, cols.stop // 2)]
            pltpu.make_async_copy(flags, flags, mask_sem.at[turn, owner]).wait()
        values = got_vis.at[owner, :, cols]
        pltpu.make_async_copy(values, values, vis_sem.at[turn, owner]).wait()

        @pl.loop(cols.start // (2 * LANES), cols.stop // (2 * LANES))
        def _(group):
            narrow = pl.ds(pl.multiple_of(group * LANES, LANES), LANES)
            wide = pl.ds(pl.multiple_of(group * 2 * LANES, 2 * LANES), 2 * LANES)
            flags = jnp.concatenate([got_mask[owner, yy, :, narrow] for yy in range(NY)], axis=0)
            kept = widen((1 - flags).astype(F32))
            high, low = split(kept * got_vis[owner, :, wide])
            out[:, wide] = dot(chosen[...], jnp.concatenate([high, low, high], axis=0))

    pieces = pl.ds(0, MODES // 2), pl.ds(MODES // 2, MODES // 2)
    sends = {}

    def send(turn, way, slot):
        piece = (way, slot, pieces[way] if slot == 0 else pl.ds(0, MODES), TURNS[turn])
        sends[turn, way, slot] = pltpu.make_async_remote_copy(
            src_ref=partial.at[piece],
            dst_ref=chain.at[piece],
            send_sem=chain_send.at[turn, way, slot],
            recv_sem=chain_sem.at[turn, way, slot],
            device_id={"chan": at(y, ahead(1 - 2 * way), core)},
            device_id_type=MESH,
        )
        sends[turn, way, slot].start()

    def begin(turn):
        cols = TURNS[turn]
        project(turn, ahead(4), partial.at[0, 0])
        partial[1, 0, MODES // 2 :, cols] = partial[0, 0, MODES // 2 :, cols]
        for way in range(2):
            send(turn, way, 0)

    def step_on(turn, slot):
        for way in range(2):
            project(turn, ahead((4 - slot) * (1 - 2 * way)), partial.at[way, slot])
            rows = pieces[way] if slot == 1 else pl.ds(0, MODES)
            cols = TURNS[turn]
            sends[turn, way, slot - 1].wait_recv()
            partial[way, slot, rows, cols] = partial[way, slot, rows, cols] + chain[way, slot - 1, rows, cols]
            send(turn, way, slot)

    def conclude(turn):
        cols = TURNS[turn]
        project(turn, z, answer, own=True)
        for way in range(2):
            sends[turn, way, 3].wait_recv()
        answer[:, cols] = (answer[:, cols] + chain[0, 3, :, cols] + chain[1, 3, :, cols]) * valid[:, cols]

        @pl.loop(0, MODES)
        def _(k):
            row = answer[pl.ds(k, 1), cols] * inverse[pl.ds(k, 1), cols]
            answer[:, cols] = answer[:, cols] - jnp.where(eye_row[:, cols] > k, gram[k, :, cols] * row, 0.0)
            answer[pl.ds(k, 1), cols] = row

        coef = coefs.at[y, z, core]
        coef[:, cols] = jnp.zeros((MODES, cols.stop - cols.start), F32)

        @pl.loop(0, MODES)
        def _(step):
            k = MODES - 1 - step
            later = jnp.sum(gram[k, :, cols] * coef[:, cols], axis=0, keepdims=True)
            coef[pl.ds(k, 1), cols] = (answer[pl.ds(k, 1), cols] - later) * inverse[pl.ds(k, 1), cols]


    def push(piece, peer, arrived, sent=None):
        pltpu.make_async_remote_copy(
            src_ref=piece,
            dst_ref=piece,
            send_sem=link_send.at[0] if sent is None else sent,
            recv_sem=arrived,
            device_id={"chan": peer},
            device_id_type=MESH,
        ).start()

    def wait(piece, arrived):
        pltpu.make_async_copy(piece, piece, arrived).wait()

    def beside(way):
        return at(y, ahead(1 - 2 * way), core)

    def finish(half, *places):
        cols = (FIRST, SECOND)[half]
        results = []
        for place in places:
            high, low = split(coefs[(*place, slice(None), cols)])
            model = dot(basis[...], jnp.concatenate([high, low, high], axis=0))
            results.append(kept_vis[at(*place), :, cols] - model)
        for place, result in zip(places, results):
            start = pl.multiple_of(at(*place) * COLS + cols.start, LANES)
            out[:, pl.ds(start, cols.stop - cols.start)] = result

    def hand(half, yy, zz, far):
        cols = (FIRST, SECOND)[half]
        push(coefs.at[yy, zz, core, :, cols], at(y, z, 1 - core), twin_sem.at[half, far], twin_send.at[0])

    def along(yy, zz, way, far):
        def go():
            push(coefs.at[yy, zz, core, :, FIRST], beside(way), along_sem.at[way, far, yy])

        if far < 4:
            go()
        elif far == 4:
            pl.when(yy % 2 == way)(go)

    def first(zz, way, far):
        if far < 4:
            push(coefs.at[y, zz, core, :, SECOND], beside(way), first_sem.at[way, far])
        elif far == 4:
            push(coefs.at[y, zz, core, :, SECOND_OF[way]], beside(way), first_sem.at[way, far])

    def above(way):
        return at((y + 1 - 2 * way + NY) % NY, z, core)

    def spread(zz):
        for way in range(2):
            push(coefs.at[y, zz, core, :, SECOND], above(way), spread_sem.at[way, zz])

    def start_second():
        pltpu.make_async_copy(kept_vis, kept_vis, load_sem.at[0]).wait()
        for way in range(2):
            first(z, way, 1)
        spread(z)
        hand(1, y, z, 0)
        finish(1, (y, z, core))

    def start_first():
        for step in (1, 3, 2):
            push(coefs.at[y, z, core, :, FIRST], at((y + step) % NY, z, core), across_sem.at[y])
        for way in range(2):
            along(y, z, way, 1)
        hand(0, y, z, 0)
        finish(0, (y, z, core))

    def origin(way, far):
        return ahead(far * (2 * way - 1))

    def second_of(far):
        if far == 4:
            zz = ahead(4)
            for way in range(2):
                wait(coefs.at[y, zz, core, :, SECOND_OF[way]], first_sem.at[way, 4])
            spread(zz)
            hand(1, y, zz, far)
            finish(1, (y, zz, core))
            return
        for way in range(2):
            zz = origin(way, far)
            wait(coefs.at[y, zz, core, :, SECOND], first_sem.at[way, far])
            first(zz, way, far + 1)
            spread(zz)
            hand(1, y, zz, far)
        finish(1, *[(y, origin(way, far), core) for way in range(2)])

    def near(far):
        return (z,) if far == 0 else (ahead(4),) if far == 4 else (ahead(far), ahead(-far))

    def second_spread(far):
        for side, zz in enumerate(near(far)):
            for way in range(2):
                yy = (y + 2 * way - 1 + NY) % NY
                wait(coefs.at[yy, zz, core, :, SECOND], spread_sem.at[way, zz])

                def relay():
                    push(coefs.at[yy, zz, core, :, SECOND], above(way), relay_sem.at[zz])

                if far in (0, 4):
                    pl.when(yy % 2 == way)(relay)
                elif side == way:
                    relay()
                hand(1, yy, zz, far)
        finish(1, *[((y + step) % NY, zz, core) for zz in near(far) for step in (1, 3)])

    def second_relay(far):
        yy = (y + 2) % NY
        for zz in near(far):
            wait(coefs.at[yy, zz, core, :, SECOND], relay_sem.at[zz])
            hand(1, yy, zz, far)
        finish(1, *[(yy, zz, core) for zz in near(far)])

    def first_across():
        @pl.loop(1, NY)
        def _(step):
            yy = (y + step) % NY
            wait(coefs.at[yy, z, core, :, FIRST], across_sem.at[yy])
            for way in range(2):
                along(yy, z, way, 1)
            hand(0, yy, z, 0)

        finish(0, *[((y + step) % NY, z, core) for step in range(1, NY)])

    def first_of(far):
        @pl.loop(0, NY)
        def _(step):
            yy = (y + step) % NY
            if far == 4:
                zz = ahead(4)
                wait(coefs.at[yy, zz, core, :, FIRST], along_sem.at[yy % 2, 4, yy])
                hand(0, yy, zz, far)
                return
            for way in range(2):
                zz = origin(way, far)
                wait(coefs.at[yy, zz, core, :, FIRST], along_sem.at[way, far, yy])
                along(yy, zz, way, far + 1)
                hand(0, yy, zz, far)

        finish(0, *[(yy, zz, core) for yy in range(NY) for zz in near(far)])

    def taken(half, far):
        amount = coefs.at[:, : len(near(far)), 0, :, (FIRST, SECOND)[half]]
        wait(amount, twin_sem.at[half, far])
        finish(half, *[(yy, zz, 1 - core) for yy in range(NY) for zz in near(far)])

    send_mask(0, 4, 3, -3)
    send_vis()
    weigh()
    make_gram()
    begin(0)
    send_mask(0, 2, -2)
    factor()
    step_on(0, 1)
    send_mask(0, 1, -1)
    send_mask(1, 4)
    step_on(0, 2)
    send_mask(1, 3, -3)
    begin(1)
    step_on(0, 3)
    send_mask(1, 2, -2)
    step_on(1, 1)
    send_mask(1, 1, -1)
    conclude(0)
    start_second()
    step_on(1, 2)
    second_of(1)
    step_on(1, 3)
    second_spread(0)
    conclude(1)
    start_first()
    second_of(2)
    second_spread(1)
    second_relay(0)
    first_across()
    second_of(3)
    first_of(1)
    second_spread(2)
    second_relay(1)
    second_of(4)
    first_of(2)
    second_spread(3)
    first_of(3)
    second_relay(2)
    taken(1, 0)
    second_spread(4)
    taken(1, 1)
    first_of(4)
    taken(0, 0)
    taken(0, 1)
    second_relay(3)
    taken(1, 2)
    taken(0, 2)
    second_relay(4)
    taken(0, 3)
    taken(1, 3)
    taken(0, 4)
    taken(1, 4)

    pltpu.make_async_copy(gram.at[: MODES - 1], gram.at[: MODES - 1], link_send.at[0]).wait()
    pltpu.make_async_copy(gram, gram, twin_send.at[0]).wait()
    for s in sends.values():
        s.wait_send()
    sent = flipped.at[:, pl.ds(0, (NX - 1) * SLAB)]
    pltpu.make_async_copy(sent, sent, send_sem.at[0]).wait()
    sent = got_mask.at[pl.ds(0, NZ - 1)]
    pltpu.make_async_copy(sent, sent, send_sem.at[1]).wait()
    sent = got_vis.at[pl.ds(0, NY * NC - 1)]
    pltpu.make_async_copy(sent, sent, send_sem.at[2]).wait()


def fit(vis, mask, modes, counts):
    outside = pl.BlockSpec(memory_space=pltpu.HBM)
    held = pl.BlockSpec(memory_space=pltpu.VMEM)
    return pl.pallas_call(
        fit_kernel,
        out_shape=jax.ShapeDtypeStruct(vis.shape, F32),
        in_specs=[outside, held, held, held],
        out_specs=held,
        scratch_shapes=[
            pltpu.VMEM((MODES, COLS), F32),
            pltpu.VMEM((1, COLS), F32),
            pltpu.VMEM((NY, NZ, NC, MODES, COLS), F32),
            pltpu.VMEM((ROWS, 3 * MODES), BF16),
            pltpu.VMEM((NY * NZ * NC, ROWS, COLS), F32),
            pltpu.VMEM((NX * SLAB, LANES), F32),
            pltpu.VMEM((NZ, NY, NC * ROWS, HALF), jnp.int32),
            pltpu.VMEM((NZ, SEL, COLS), F32),
            pltpu.VMEM((NX * SLAB, COLS), BF16),
            pltpu.VMEM((MODES, MODES, COLS), F32),
            pltpu.VMEM((MODES, NX * SLAB), F32),
            pltpu.VMEM((MODES, 3 * SEL), BF16),
            pltpu.VMEM((2, 4, MODES, COLS), F32),
            pltpu.VMEM((2, 4, MODES, COLS), F32),
            pltpu.VMEM((MODES, COLS), F32),
            pltpu.SemaphoreType.DMA((1,)),
            pltpu.SemaphoreType.DMA((2, NZ)),
            pltpu.SemaphoreType.DMA((2, NZ)),
            pltpu.SemaphoreType.DMA((2, 2, 4)),
            pltpu.SemaphoreType.DMA((3,)),
            pltpu.SemaphoreType.DMA((2, 2, 4)),
            pltpu.SemaphoreType.DMA((NY,)),
            pltpu.SemaphoreType.DMA((2, 5, NY)),
            pltpu.SemaphoreType.DMA((2, 5)),
            pltpu.SemaphoreType.DMA((2, NZ)),
            pltpu.SemaphoreType.DMA((NZ,)),
            pltpu.SemaphoreType.DMA((2, 5)),
            pltpu.SemaphoreType.DMA((1,)),
            pltpu.SemaphoreType.DMA((1,)),
            pltpu.SemaphoreType.DMA((1,)),
        ],
        compiler_params=pltpu.CompilerParams(
            collective_id=0, has_side_effects=True, vmem_limit_bytes=44 * 1024 * 1024
        ),
        name="fit",
    )(vis, mask, modes, counts)


def per_device(visibility, interference_mask, valid_time_count, fit_modes):
    mask = interference_mask.reshape(NY, NZ, NC * ROWS, HALF)
    return fit(visibility, mask, fit_modes.T, valid_time_count.reshape(1, -1))


def solution(mesh):
    placed = (P("chan", "grp"), P(None, ("grp", "chan")), P(("grp", "chan")), P("grp", None))
    return jax.shard_map(
        per_device, mesh=mesh, in_specs=placed, out_specs=P("chan", "grp"), check_vma=False
    )
```
